512 devices in a mesh: expert: 8 (over x, core), shard: 64 (over y, z).
Axes of the slice: x: 4, y: 8, z: 8, core: 2. Of those that a mesh axis runs over, the one named last changes fastest.
Arguments:
- tokens: bfloat16 [384, 4096], P('shard', 'expert'), may hold values from -6 to 6
- expert_ids: int32 [384, 2], P('shard'), may hold values from 0 to 7, all different within a row; in each aligned block of 6 rows (0 to 5, 6 to 11, ...) at most 3 rows name the same one
- gates: float32 [384, 2], P('shard'), may hold values from 0.1 to 1
- gate_proj: bfloat16 [8, 4096, 8192], P('expert', None, 'shard'), may hold values from -0.09375 to 0.09375
- up_proj: bfloat16 [8, 4096, 8192], P('expert', None, 'shard'), may hold values from -0.09375 to 0.09375
- down_proj_t: bfloat16 [8, 4096, 8192], P('expert', 'shard'), may hold values from -0.0625 to 0.0625
Outputs:
- mixed: bfloat16 [384, 4096], P('shard', 'expert')
The draws below stay inside these ranges and needn't reach their ends.
Inputs may be any that keep to these rules, and one draw needn't show every extreme that they name: `expert_ids`: each token names two different experts; among the 6 tokens of one aligned block no expert is named more than 3 times, and in every draw some expert is named exactly 3 times in some block.
All inputs are finite; a program needn't handle non-finite values.
Results may differ from the reference program's by a relative error of at most 0.0085.
Values may be sent and summed in bfloat16 or wider, within the bound.
A program may use at most 64 MiB of HBM per device.

```python
import math
import jax
import jax.numpy as jnp
import numpy as np
from jax import lax

D = 4096
FF = 8192
TOK_SH = 6
EXPERTS = 8
CAP = 3
TOKENS = 384
N_SHARD = 64


def shard_levels(own_key, extent, pieces, least, top_value):
    gain = 1.0
    for dim, parts in pieces:
        heights = jax.random.uniform(jax.random.fold_in(jax.random.fold_in(own_key, 6), dim), (parts,), jnp.float32, least / len(pieces), top_value / len(pieces))
        gain = gain * jnp.repeat(jnp.exp(heights), extent[dim] // parts).reshape((-1,) + (1,) * (len(extent) - 1 - dim))
    return gain


def deal_out(rng, own, number, rows, count, top, bound, slope):
    sequence = jax.random.permutation(rng, count)
    crowded, usual = shares(count, rows * top, bound, slope, True), shares(count, rows * top, bound, slope, False)
    places = jnp.arange(count)

    def named(lengths, offset_by):
        used = int((lengths > 0).sum())
        fixed = max(1, used // 4)
        passed = fixed + (places - fixed + offset_by * (used - fixed)) % max(1, count - fixed)
        return jnp.zeros((count,), jnp.int32).at[sequence[jnp.where(places < fixed, places, passed)]].set(jnp.asarray(lengths, jnp.int32))

    lengths = jnp.where(number % 4 == 0, named(crowded, number // 4), named(usual, number - number // 4 - 1))
    mixed = jax.random.permutation(jax.random.fold_in(own, 3), count)
    source_of, taker = mixed[0:count // 2 * 2:2], mixed[1:count // 2 * 2:2]
    room = jnp.minimum(lengths[source_of] - 1, bound - lengths[taker]) // 2
    room = jnp.where((source_of == sequence[0]) | (taker == sequence[0]) | (lengths[taker] == 0), 0, jnp.maximum(room, 0))
    passed = jax.random.randint(jax.random.fold_in(own, 4), (count // 2,), 0, 1 << 20) % (room + 1)
    lengths = lengths.at[source_of].add(-passed).at[taker].add(passed)
    labels = jnp.searchsorted(jnp.cumsum(lengths), jnp.arange(rows * top), side="right").astype(jnp.int32)
    table = labels.reshape(top, rows).T
    table = table[jax.random.permutation(jax.random.fold_in(own, 1), rows)]
    offset_by = jax.random.randint(jax.random.fold_in(own, 2), (rows, 1), 0, top)
    return jnp.take_along_axis(table, (jnp.arange(top)[None, :] + offset_by) % top, axis=1)


def shares(number_of, total, most, skew, full):
    weights = [(1 << 20) // math.isqrt(standing ** skew) + 1 for standing in range(1, number_of + 1)]
    largest = most if full else min(most, max(-(-total // number_of), total * weights[0] // sum(weights)))
    least = 1 if total - largest >= number_of - 1 else 0
    given, surplus = [largest] + [least] * (number_of - 1), total - largest - least * (number_of - 1)
    while surplus > 0:
        free = [i for i in range(1, number_of) if given[i] < largest] or [i for i in range(1, number_of) if given[i] < most]
        pool, left = sum([weights[i] for i in free]), surplus
        for i in free:
            more = min(most - given[i], max(1, left * weights[i] // pool), surplus)
            given[i] = given[i] + more
            surplus = surplus - more
    return np.array(given)


def noise(key, extent, spread, reach, shards=(), held_as=jnp.bfloat16):
    array = jax.random.normal(key, extent, jnp.float32) * spread
    if len(shards) > 0:
        array = shard_levels(key, extent, shards, -0.22, 0.18) * array
    return jnp.clip(array, min=-reach, max=reach).astype(held_as)


def setup_inputs(seed: int = 0) -> dict:
    key_list = jax.random.split(jax.random.key(seed), 7)
    tokens = noise(key_list[0], (TOKENS, D), 1.0, 6.0, ((0, 64), (1, 8)))
    expert_ids_keys = jax.random.split(jax.random.fold_in(key_list[1], 1), TOKENS // TOK_SH)
    expert_ids_turns = jax.random.permutation(jax.random.fold_in(key_list[1], 3), TOKENS // TOK_SH)
    expert_ids = jax.vmap(lambda own, number: deal_out(jax.random.fold_in(key_list[1], 2), own, number, TOK_SH, EXPERTS, 2, CAP, 2))(expert_ids_keys, expert_ids_turns).reshape((TOKENS, 2))
    gates = jnp.clip(jnp.exp(math.log(1.0) - 2.3025851 * jax.random.uniform(key_list[2], (TOKENS, 2), jnp.float32) ** shard_levels(key_list[2], (TOKENS, 2), ((0, 64),), -0.2, 0.2)), 0.1, 1.0)
    gate_proj = noise(key_list[3], (EXPERTS, D, FF), D ** -0.5, 0.09375, ((0, 8), (2, 64)))
    up_proj = noise(key_list[4], (EXPERTS, D, FF), D ** -0.5, 0.09375, ((0, 8), (2, 64)))
    down_proj_t = noise(key_list[5], (EXPERTS, D, FF), FF ** -0.5, 0.0625, ((0, 8), (1, 64)))
    return dict(tokens=tokens, expert_ids=expert_ids, gates=gates, gate_proj=gate_proj, up_proj=up_proj, down_proj_t=down_proj_t)


def reference(tokens, expert_ids, gates, gate_proj, up_proj, down_proj_t):
    expert_range = jnp.arange(EXPERTS, dtype=jnp.int32)
    matches = expert_ids[:, :, None] == expert_range[None, None, :]
    routed = jnp.sum(matches.astype(jnp.int32), axis=1)
    weight = jnp.sum(gates[:, :, None] * matches.astype(jnp.float32), axis=1)
    blocked = routed.reshape(N_SHARD, TOK_SH, EXPERTS)
    slot_rank = (jnp.cumsum(blocked, axis=1) - blocked).reshape(TOKENS, EXPERTS)
    token_block = jnp.arange(TOKENS, dtype=jnp.int32) // TOK_SH
    target = token_block[:, None] * CAP + slot_rank
    row_ids = jnp.arange(N_SHARD * CAP, dtype=jnp.int32)
    mixed_sum = jnp.zeros((TOKENS, D), jnp.float32)
    for expert in range(EXPERTS):
        picker = ((target[:, expert][None, :] == row_ids[:, None]) & (routed[:, expert][None, :] > 0)).astype(jnp.float32)
        picked = jnp.dot(picker.astype(jnp.bfloat16), tokens, preferred_element_type=jnp.float32).astype(jnp.bfloat16)
        gate_out = jnp.dot(picked, gate_proj[expert], preferred_element_type=jnp.float32)
        up_out = jnp.dot(picked, up_proj[expert], preferred_element_type=jnp.float32)
        hidden = (jax.nn.silu(gate_out) * up_out).astype(jnp.bfloat16)
        expert_out = lax.dot_general(hidden, down_proj_t[expert], (((1,), (1,)), ((), ())), preferred_element_type=jnp.float32).astype(jnp.bfloat16)
        combiner = picker.T * weight[:, expert][:, None]
        mixed_sum = mixed_sum + jnp.dot(combiner, expert_out.astype(jnp.float32), precision=lax.Precision.HIGHEST)
    return mixed_sum.astype(jnp.bfloat16)
```

```python
import functools

import jax
import jax.numpy as jnp
from jax import lax
from jax.experimental import pallas as pl
from jax.experimental.pallas import tpu as pltpu
from jax.sharding import Mesh
from jax.sharding import PartitionSpec as P

SHARD = ("shard_0", "shard_1")
MESH = pl.DeviceIdType.MESH
NARROW = ("shard_1", "shard_0")
WIDE = ("shard_0", "shard_1")
CHUNKS = 4


def loop(count, body):
    lax.fori_loop(0, count, lambda i, c: (body(i), c)[1], 0)


def kernel(
    n, cap, half, hidden_units,
    msg_ref, comb_ref, gate_hbm, up_hbm, down_hbm, out_ref,
    toks, sel, rows, part, hid, acc, give, got, back, gate_w, up_w, down_w,
    load_sem, a1_send, a1_recv, a2_send, a2_recv, a3_send, a3_recv,
    c1_send, c1_recv, c2_send, c2_recv, e1_send, e1_recv, e2_send, e2_recv,
):
    e = lax.axis_index("expert")
    y = lax.axis_index("shard_0")
    z = lax.axis_index("shard_1")
    nar = (z, y)
    wid = (y, z)
    top = n // 2
    line = n * cap
    total = n * line
    hrows = total // 2
    groups = line // 8
    per = n // CHUNKS if n >= CHUNKS else 1
    chunks = n // per

    def plus(a, b):
        return lax.rem(a + b + n, n)

    loads = [
        pltpu.make_async_copy(gate_hbm, gate_w, load_sem.at[0]),
        pltpu.make_async_copy(up_hbm, up_w, load_sem.at[1]),
        pltpu.make_async_copy(down_hbm, down_w.at[0], load_sem.at[2]),
        pltpu.make_async_copy(down_hbm, down_w.at[1], load_sem.at[3]),
    ]
    for copy in loads:
        copy.start()

    barrier = pltpu.get_barrier_semaphore()
    for axis, own in (("expert", e), ("shard_0", y), ("shard_1", z)):
        for d in range(1, n):
            pl.semaphore_signal(
                barrier, inc=1, device_id={axis: plus(own, d)}, device_id_type=MESH
            )
    pl.semaphore_wait(barrier, 3 * (n - 1))

    def a1(h, d):
        return pltpu.make_async_remote_copy(
            src_ref=msg_ref.at[h],
            dst_ref=toks.at[h, nar[h]],
            send_sem=a1_send.at[h, d],
            recv_sem=a1_recv.at[h, d],
            device_id={NARROW[h]: plus(nar[h], -d)},
            device_id_type=MESH,
        )

    for d in range(1, n):
        for h in range(2):
            a1(h, d).start()
    for h in range(2):
        toks[h, nar[h]] = msg_ref[h]

    def a2(h, d):
        return pltpu.make_async_remote_copy(
            src_ref=sel.at[h, plus(e, -d)],
            dst_ref=rows.at[h, wid[h], d],
            send_sem=a2_send.at[h, d],
            recv_sem=a2_recv.at[h, d],
            device_id={"expert": plus(e, -d)},
            device_id_type=MESH,
        )

    lanes = 8 * n
    row_of = lax.broadcasted_iota(jnp.int32, (line, 128), 0)
    lane_of = lax.broadcasted_iota(jnp.int32, (line, 128), 1)
    same_block = (row_of // cap) == (lane_of // 8)
    rank_of = (row_of % cap + 1).astype(jnp.float32)
    for h in range(2):
        for d in range(1, n):
            a1(h, d).wait_recv()
        codes = jnp.zeros((8, 128), jnp.float32)
        for b in range(n):
            codes = codes + toks[h, b, :, half:].astype(jnp.float32)
        feats = toks[h, :, :, :half].reshape(lanes, half)
        for k in range(n):
            hit = same_block & (codes[k : k + 1, :] == rank_of)
            pick = jnp.where(hit, 1.0, 0.0).astype(jnp.bfloat16)[:, :lanes]
            found = jnp.dot(pick, feats, preferred_element_type=jnp.float32)
            sel[h, k] = found.reshape(groups, 8, half).astype(jnp.bfloat16)
        for d in range(1, n):
            a2(h, d).start()
        rows[h, wid[h], 0] = sel[h, e]

    def a3(h, way, k, j):
        step = 1 if way == 0 else -1
        unit = rows.at[h, plus(wid[h], -step * (k - 1)), pl.ds(j * per, per)]
        return pltpu.make_async_remote_copy(
            src_ref=unit,
            dst_ref=unit,
            send_sem=a3_send.at[h, way, k - 1, j],
            recv_sem=a3_recv.at[h, way, k - 1, j],
            device_id={WIDE[h]: plus(wid[h], step)},
            device_id_type=MESH,
        )

    def split(way, k, j, count):
        return k < top or (j < count // 2) == (way == 0)

    for j in range(chunks):
        for h in range(2):
            for d in range(j * per, (j + 1) * per):
                if d > 0:
                    a2(h, d).wait_recv()
            for way in range(2):
                if split(way, 1, j, chunks):
                    a3(h, way, 1, j).start()
    for k in range(1, top + 1):
        for j in range(chunks):
            for h in range(2):
                for way in range(2):
                    if split(way, k, j, chunks):
                        a3(h, way, k, j).wait_recv()
                    if k < top and split(way, k + 1, j, chunks):
                        a3(h, way, k + 1, j).start()

    for copy in loads:
        copy.wait()
    for h in range(2):
        part[h] = jnp.zeros((total, 2 * hidden_units), jnp.float32)

        def project(d, h=h):
            at = pl.multiple_of(plus(e, d) * (2 * half) + h * half, half)
            lhs = rows[h, :, d].reshape(total, half)
            rhs = jnp.concatenate([gate_w[pl.ds(at, half), :], up_w[pl.ds(at, half), :]], axis=1)
            part[h] += jnp.dot(lhs, rhs, preferred_element_type=jnp.float32)

        loop(n, project)
    for a in range(n):
        for b in range(n):
            to, at = a * line + b * cap, b * line + a * cap
            part[1, to : to + cap, :] += part[0, at : at + cap, :]
    both = part[1]
    gated = both[:, :hidden_units]
    hidden = ((gated / (1.0 + jnp.exp(-gated))) * both[:, hidden_units:]).astype(jnp.bfloat16)
    for h in range(2):
        hid[h, wid[h], 0] = hidden[h * hrows : (h + 1) * hrows, :]

    def c1(h, d):
        return pltpu.make_async_remote_copy(
            src_ref=hid.at[h, wid[h], 0],
            dst_ref=hid.at[h, wid[h], d],
            send_sem=c1_send.at[h, d],
            recv_sem=c1_recv.at[h, d],
            device_id={NARROW[h]: plus(nar[h], -d)},
            device_id_type=MESH,
        )

    order = [0]
    for d in range(1, top):
        order += [d, n - d]
    order.append(top)
    for d in order[1:]:
        for h in range(2):
            c1(h, d).start()

    def c2(h, way, k, d):
        step = 1 if way == 0 else -1
        unit = hid.at[h, plus(wid[h], -step * (k - 1)), d]
        return pltpu.make_async_remote_copy(
            src_ref=unit,
            dst_ref=unit,
            send_sem=c2_send.at[h, way, k - 1, d],
            recv_sem=c2_recv.at[h, way, k - 1, d],
            device_id={WIDE[h]: plus(wid[h], step)},
            device_id_type=MESH,
        )

    acc[...] = jnp.zeros_like(acc)

    def use(h, src, pair):
        lhs, rhs = [], []
        for d in pair:
            other = plus(nar[h], d)
            unit = src * n + other if h == 0 else other * n + src
            at = pl.multiple_of(unit * hidden_units, hidden_units)
            lhs.append(hid[h, src, d])
            rhs.append(down_w[:, :, pl.ds(at, hidden_units)].reshape(128, hidden_units))
        acc[h] += lax.dot_general(
            jnp.concatenate(lhs, axis=1),
            jnp.concatenate(rhs, axis=1),
            (((1,), (1,)), ((), ())),
            preferred_element_type=jnp.float32,
        )

    for j, d in enumerate(order):
        for h in range(2):
            if d > 0:
                c1(h, d).wait_recv()
            for way in range(2):
                if split(way, 1, j, n):
                    c2(h, way, 1, d).start()
    for k in range(1, top + 1):
        for i in range(n // 2):
            pair = order[2 * i : 2 * i + 2]
            for h in range(2):
                for way in range(2):
                    for j in (2 * i, 2 * i + 1):
                        if split(way, k, j, n):
                            c2(h, way, k, order[j]).wait_recv()
                        if k < top and split(way, k + 1, j, n):
                            c2(h, way, k + 1, order[j]).start()
            for h in range(2):
                if k == 1:
                    use(h, wid[h], pair)
                else:
                    use(h, plus(wid[h], -(k - 1)), pair)
                    use(h, plus(wid[h], k - 1), pair)
    for i in range(n // 2):
        for h in range(2):
            use(h, plus(wid[h], top), order[2 * i : 2 * i + 2])

    for a in range(n):
        for b in range(n):
            at = (a % top) * line + b * cap
            give[a, b] = acc[a // top, at : at + cap, :].astype(jnp.bfloat16)

    def e1(d):
        return pltpu.make_async_remote_copy(
            src_ref=give.at[plus(z, -d)],
            dst_ref=got.at[z],
            send_sem=e1_send.at[d],
            recv_sem=e1_recv.at[d],
            device_id={"shard_1": plus(z, -d)},
            device_id_type=MESH,
        )

    for d in range(1, n):
        e1(d).start()
    got[z] = give[z]
    for d in range(1, n):
        e1(d).wait_recv()

    def e2(b, src):
        return pltpu.make_async_remote_copy(
            src_ref=got.at[:, b],
            dst_ref=back.at[src],
            send_sem=e2_send.at[b],
            recv_sem=e2_recv.at[src],
            device_id={"expert": y, "shard_0": b},
            device_id_type=MESH,
        )

    for b in range(n):
        here = (e == y) & (y == b)

        @pl.when(jnp.logical_not(here))
        def _(b=b):
            e2(b, e).start()

        @pl.when(here)
        def _(b=b):
            back[e] = got[:, b]

    for src in range(n):

        @pl.when(jnp.logical_not((src == e) & (y == e)))
        def _(src=src):
            e2(0, src).wait_recv()

    coefs = comb_ref[...]
    low = lax.broadcasted_iota(jnp.int32, (cap, 128), 1) < 64
    sums = [jnp.zeros((8, 128), jnp.float32) for _ in range(n // 2)]
    for src in range(n):
        for m in range(n // 2):
            value = jnp.where(
                low,
                back[src, 2 * m].astype(jnp.float32),
                back[src, 2 * m + 1].astype(jnp.float32),
            )
            for s in range(cap):
                at = src * cap + s
                sums[m] = sums[m] + coefs[:, at : at + 1] * value[s : s + 1, :]
    for m in range(n // 2):
        out_ref[:, m * 128 : (m + 1) * 128] = sums[m][: out_ref.shape[0], :].astype(jnp.bfloat16)

    for h in range(2):
        for d in range(1, n):
            a1(h, d).wait_send()
            a2(h, d).wait_send()
            c1(h, d).wait_send()
        for way in range(2):
            for k in range(1, top + 1):
                for j in range(chunks):
                    if split(way, k, j, chunks):
                        a3(h, way, k, j).wait_send()
                for j in range(n):
                    if split(way, k, j, n):
                        c2(h, way, k, order[j]).wait_send()
    for d in range(1, n):
        e1(d).wait_send()
    for b in range(n):

        @pl.when(jnp.logical_not((e == y) & (y == b)))
        def _(b=b):
            e2(b, e).wait_send()


def shards(n, tokens, expert_ids, gates, gate_proj, up_proj, down_proj_t):
    tok_count, feats = tokens.shape
    half = feats // 2
    hidden_units = gate_proj.shape[2]
    out_feats = down_proj_t.shape[1]
    cap = min(tok_count, 4 * tok_count // n)
    y, z = lax.axis_index("shard_0"), lax.axis_index("shard_1")
    expert_range = jnp.arange(n, dtype=jnp.int32)
    matches = expert_ids[:, :, None] == expert_range[None, None, :]
    routed = jnp.sum(matches.astype(jnp.int32), axis=1)
    weight = jnp.sum(gates[:, :, None] * matches.astype(jnp.float32), axis=1)
    rank = jnp.cumsum(routed, axis=0) - routed
    code = jnp.where(routed > 0, rank + 1, 0)
    slot = jnp.arange(cap, dtype=jnp.int32)
    picked = jnp.where(code[:, :, None] == slot[None, None, :] + 1, weight[:, :, None], 0.0)
    comb = jnp.pad(
        picked.reshape(tok_count, n * cap), ((0, 8 - tok_count), (0, 128 - n * cap))
    )
    lane = jnp.arange(128, dtype=jnp.int32)
    tok = jnp.arange(tok_count, dtype=jnp.int32)
    msgs = []
    for h, at in enumerate((z, y)):
        place = lane[None, :] == at * 8 + tok[:, None]
        meta = jnp.sum(jnp.where(place[:, None, :], code[:, :, None], 0), axis=0)
        meta = jnp.pad(meta, ((0, 8 - n), (0, 0))).astype(jnp.bfloat16)
        body = jnp.pad(tokens[:, h * half : (h + 1) * half], ((0, 8 - tok_count), (0, 0)))
        msgs.append(jnp.concatenate([body, meta], axis=1))
    msg = jnp.stack(msgs)

    line = n * cap
    total = n * line
    bf16 = jnp.bfloat16
    per = n // CHUNKS if n >= CHUNKS else 1
    dma = pltpu.SemaphoreType.DMA
    vmem, hbm = pltpu.VMEM, pl.ANY
    return pl.pallas_call(
        functools.partial(kernel, n, cap, half, hidden_units),
        out_shape=jax.ShapeDtypeStruct((tok_count, feats), bf16),
        in_specs=[
            pl.BlockSpec(memory_space=vmem),
            pl.BlockSpec(memory_space=vmem),
            pl.BlockSpec(memory_space=hbm),
            pl.BlockSpec(memory_space=hbm),
            pl.BlockSpec(memory_space=hbm),
        ],
        out_specs=pl.BlockSpec(memory_space=vmem),
        scratch_shapes=[
            vmem((2, n, 8, half + 128), bf16),
            vmem((2, n, line // 8, 8, half), bf16),
            vmem((2, n, n, line // 8, 8, half), bf16),
            vmem((2, total, 2 * hidden_units), jnp.float32),
            vmem((2, n, n, total // 2, hidden_units), bf16),
            vmem((2, total // 2, 128), jnp.float32),
            vmem((n, n, cap, 128), bf16),
            vmem((n, n, cap, 128), bf16),
            vmem((n, n, cap, 128), bf16),
            vmem(gate_proj.shape[1:], bf16),
            vmem(up_proj.shape[1:], bf16),
            vmem((2, out_feats, down_proj_t.shape[2]), bf16),
            dma((4,)),
            dma((2, n)), dma((2, n)),
            dma((2, n)), dma((2, n)),
            dma((2, 2, n // 2, n // per)), dma((2, 2, n // 2, n // per)),
            dma((2, n)), dma((2, n)),
            dma((2, 2, n // 2, n)), dma((2, 2, n // 2, n)),
            dma((n,)), dma((n,)),
            dma((n,)), dma((n,)),
        ],
        compiler_params=pltpu.CompilerParams(collective_id=0, has_side_effects=True),
        name="experts",
    )(msg, comb, gate_proj[0], up_proj[0], down_proj_t[0])


def solution(mesh):
    n = mesh.shape["expert"]
    split = Mesh(mesh.devices.reshape(n, n, n), ("expert", "shard_0", "shard_1"))
    placed = (
        P(SHARD, "expert"),
        P(SHARD, None),
        P(SHARD, None),
        P("expert", None, SHARD),
        P("expert", None, SHARD),
        P("expert", SHARD, None),
    )
    return jax.shard_map(
        functools.partial(shards, n),
        mesh=split,
        in_specs=placed,
        out_specs=P(SHARD, "expert"),
        check_vma=False,
    )
```

```python
import functools

import jax
import jax.numpy as jnp
from jax import lax
from jax.experimental import pallas as pl
from jax.experimental.pallas import tpu as pltpu
from jax.sharding import Mesh
from jax.sharding import PartitionSpec as P

SHARD = ("shard_0", "shard_1")
MESH = pl.DeviceIdType.MESH
NARROW = ("shard_1", "shard_0")
WIDE = ("shard_0", "shard_1")
CHUNKS = 2
SPAN = 64
F32, BF16 = jnp.float32, jnp.bfloat16


def kernel(
    n, cap, tok_hbm, ids_hbm, gates_hbm, gate_hbm, up_hbm, down_hbm, out_ref,
    tok_v, ids_v, gates_v, stage, toks, sel, rows, part, hid, acc, give, got, got32, pass_on, back,
    gate_w, up_w, down_w,
    load_sem, a1_send, a1_recv, a2_send, a2_recv, a3_send, a3_recv,
    c1_send, c1_recv, c2_send, c2_recv, e1_send, e1_recv, e2_send, e2_recv,
):
    e = lax.axis_index("expert")
    y = lax.axis_index("shard_0")
    z = lax.axis_index("shard_1")
    nar = (z, y)
    wid = (y, z)
    top = n // 2
    cells = n * n
    hcells = cells // 2
    tok_count, feats = tok_v.shape
    half = feats // 2
    hidden_units = gate_w.shape[1]
    per = n // CHUNKS
    far = [d for k in range(top) for d in sorted({top - k, top + k}) if d < n]

    def plus(a, b):
        return lax.rem(a + b + n, n)

    small = [
        pltpu.make_async_copy(ids_hbm, ids_v, load_sem.at[0]),
        pltpu.make_async_copy(gates_hbm, gates_v, load_sem.at[1]),
        pltpu.make_async_copy(tok_hbm, tok_v, load_sem.at[2]),
    ]
    loads = [
        pltpu.make_async_copy(gate_hbm, gate_w, load_sem.at[3]),
        pltpu.make_async_copy(up_hbm, up_w, load_sem.at[4]),
        pltpu.make_async_copy(down_hbm, down_w.at[0], load_sem.at[5]),
        pltpu.make_async_copy(down_hbm, down_w.at[1], load_sem.at[6]),
    ]
    for copy in small:
        copy.start()
    barrier = pltpu.get_barrier_semaphore()
    for d in far:
        for axis, own in (("shard_1", z), ("shard_0", y), ("expert", e)):
            pl.semaphore_signal(
                barrier, inc=1, device_id={axis: plus(own, d)}, device_id_type=MESH
            )
    for copy in small:
        copy.wait()
    for copy in loads:
        copy.start()

    ids = [[ids_v[k : k + 1, t : t + 1] for t in range(tok_count)] for k in range(2)]
    amount = [[gates_v[k : k + 1, t : t + 1] for t in range(tok_count)] for k in range(2)]

    def codes_of(expert):
        run = jnp.zeros(expert.shape, F32)
        out = []
        for t in range(tok_count):
            hit = (ids[0][t] == expert) | (ids[1][t] == expert)
            out.append(jnp.where(hit, run + 1.0, 0.0))
            run = run + jnp.where(hit, 1.0, 0.0)
        return out

    sub = lax.broadcasted_iota(jnp.int32, (8, half), 0)
    lane = lax.broadcasted_iota(jnp.int32, (8, half), 1)
    held = half // SPAN
    expert = jnp.where(sub >= 6, (sub - 6) * held + lane // SPAN, -1)
    codes = codes_of(expert)
    stage[...] = jnp.zeros_like(stage)
    stage[0:tok_count, :] = tok_v[...].astype(F32)
    for h in range(2):
        here = (lane % SPAN) // 8 == nar[h]
        spare = jnp.zeros((8, half), F32)
        for t in range(tok_count):
            spare = jnp.where(here & (lane % 8 == t), codes[t], spare)
        toks[h, nar[h]] = (stage[:, h * half : (h + 1) * half] + spare).astype(BF16)

    pl.semaphore_wait(barrier, 3 * (n - 1))

    def a1(h, d):
        block = toks.at[h, nar[h]]
        return pltpu.make_async_remote_copy(
            src_ref=block,
            dst_ref=block,
            send_sem=a1_send.at[h, d],
            recv_sem=a1_recv.at[h, d],
            device_id={NARROW[h]: plus(nar[h], -d)},
            device_id_type=MESH,
        )

    for d in far:
        for h in range(2):
            a1(h, d).start()

    def a2(h, d):
        return pltpu.make_async_remote_copy(
            src_ref=sel.at[h, plus(e, -d)],
            dst_ref=rows.at[h, :, wid[h], d],
            send_sem=a2_send.at[h, d],
            recv_sem=a2_recv.at[h, d],
            device_id={"expert": plus(e, -d)},
            device_id_type=MESH,
        )

    m = held * cap * n
    row_of = lax.broadcasted_iota(jnp.int32, (m, half), 0)
    lane_of = lax.broadcasted_iota(jnp.int32, (m, half), 1)
    meets = ((lane_of % SPAN) // 8 == row_of % n) & (lane_of // SPAN == row_of // (cap * n))
    wanted = jnp.where(meets, ((row_of // n) % cap + 1).astype(F32), -1.0)
    for h in range(2):
        for d in far:
            a1(h, d).wait_recv()
        marks = jnp.zeros((8, half), F32)
        for b in range(n):
            marks = marks + toks[h, b].astype(F32)
        block = toks[h].reshape(8 * n, half)
        if 8 * n < SPAN:
            block = jnp.concatenate([block, jnp.zeros((SPAN - 8 * n, half), BF16)], axis=0)
        block = jnp.concatenate([block] * held, axis=0)
        pick = jnp.concatenate(
            [jnp.where(marks[6 + r : 7 + r, :] == wanted, 1.0, 0.0) for r in range(n // held)],
            axis=0,
        ).astype(BF16)
        found = jnp.dot(pick, block, preferred_element_type=F32)
        sel[h] = found.reshape(n, cap, n, half).astype(BF16)
        for d in range(1, n):
            a2(h, d).start()
        rows[h, :, wid[h], 0] = sel[h, e]

    def a3(h, s, way, k, j):
        step = 1 if way == 0 else -1
        unit = rows.at[h, s, plus(wid[h], -step * (k - 1)), pl.ds(j * per, per)]
        return pltpu.make_async_remote_copy(
            src_ref=unit,
            dst_ref=unit,
            send_sem=a3_send.at[h, s, way, k - 1, j],
            recv_sem=a3_recv.at[h, s, way, k - 1, j],
            device_id={WIDE[h]: plus(wid[h], step)},
            device_id_type=MESH,
        )

    def split(way, k, j, count):
        return k < top or (j < count // 2) == (way == 0)

    for j in range(CHUNKS):
        for h in range(2):
            for d in range(j * per, (j + 1) * per):
                if d > 0:
                    a2(h, d).wait_recv()
        for s in range(cap):
            for h in range(2):
                for way in range(2):
                    if split(way, 1, j, CHUNKS):
                        a3(h, s, way, 1, j).start()

    order = [0]
    for d in range(1, top):
        order += [d, n - d]
    order.append(top)
    place = {d: p for p, d in enumerate(order)}

    def c1(h, s, way, k):
        step = -1 if way == 0 else 1
        return pltpu.make_async_remote_copy(
            src_ref=hid.at[h, s, wid[h], place[(-step * (k - 1)) % n]],
            dst_ref=hid.at[h, s, wid[h], place[(-step * k) % n]],
            send_sem=c1_send.at[h, s, way, k - 1],
            recv_sem=c1_recv.at[h, s, way, k - 1],
            device_id={NARROW[h]: plus(nar[h], step)},
            device_id_type=MESH,
        )

    def in_line(s, way, k):
        return k < top or way == s % 2

    def c2(h, s, way, k, i):
        step = 1 if way == 0 else -1
        unit = hid.at[h, s, plus(wid[h], -step * (k - 1)), pl.ds(2 * i, 2)]
        return pltpu.make_async_remote_copy(
            src_ref=unit,
            dst_ref=unit,
            send_sem=c2_send.at[h, s, way, k - 1, i],
            recv_sem=c2_recv.at[h, s, way, k - 1, i],
            device_id={WIDE[h]: plus(wid[h], step)},
            device_id_type=MESH,
        )

    def project(s):
        sums = []
        for h in range(2):
            total = jnp.zeros((cells, 2 * hidden_units), F32)
            for d in range(n):
                at = pl.multiple_of(plus(e, d) * (2 * half) + h * half, half)
                lhs = rows[h, s, :, d].reshape(cells, half)
                rhs = jnp.concatenate(
                    [gate_w[pl.ds(at, half), :], up_w[pl.ds(at, half), :]], axis=1
                )
                total = total + jnp.dot(lhs, rhs, preferred_element_type=F32)
            sums.append(total)
        for c in range(2):
            part[c] = sums[0][:, c * hidden_units : (c + 1) * hidden_units]
        gated, up = (
            jnp.concatenate([part[c, pl.ds(b, n, stride=n), :] for b in range(n)], axis=0)
            + sums[1][:, c * hidden_units : (c + 1) * hidden_units]
            for c in range(2)
        )
        hidden = ((gated / (1.0 + jnp.exp(-gated))) * up).astype(BF16)
        for h in range(2):
            hid[h, s, wid[h], 0] = hidden[h * hcells : (h + 1) * hcells, :]

    for k in range(1, top + 1):
        if k == top:
            for copy in loads:
                copy.wait()
        for s in range(cap):
            for j in range(CHUNKS):
                for h in range(2):
                    for way in range(2):
                        if split(way, k, j, CHUNKS):
                            a3(h, s, way, k, j).wait_recv()
                        if k < top and split(way, k + 1, j, CHUNKS):
                            a3(h, s, way, k + 1, j).start()
            if k == top:
                project(s)
                for h in range(2):
                    for way in range(2):
                        if in_line(s, way, 1):
                            c1(h, s, way, 1).start()

    acc[...] = jnp.zeros_like(acc)
    pairs = n // 2

    def use(h, src, i):
        lhs, rhs = [], []
        for p in (2 * i, 2 * i + 1):
            other = plus(nar[h], order[p])
            unit = src * n + other if h == 0 else other * n + src
            at = pl.multiple_of(unit * hidden_units, hidden_units)
            lhs.append(hid[h, :, src, p].reshape(cap * hcells, hidden_units))
            rhs.append(down_w[:, :, pl.ds(at, hidden_units)].reshape(128, hidden_units))
        acc[h] += lax.dot_general(
            jnp.concatenate(lhs, axis=1),
            jnp.concatenate(rhs, axis=1),
            (((1,), (1,)), ((), ())),
            preferred_element_type=F32,
        )

    def use_slot(slot):
        for h in range(2):
            if 1 <= slot <= pairs:
                use(h, wid[h], slot - 1)
            for i in range(pairs):
                k = slot - 1 - i
                if 1 <= k < top:
                    use(h, plus(wid[h], -k), i)
                    use(h, plus(wid[h], k), i)
                elif k == top:
                    use(h, plus(wid[h], k), i)

    last = pairs + top
    for slot in range(1, last + 1):
        if slot == last:
            use_slot(slot - 1)
        for s in range(cap):
            for h in range(2):
                if slot <= top:
                    for way in range(2):
                        if in_line(s, way, slot):
                            c1(h, s, way, slot).wait_recv()
                        if slot < top and in_line(s, way, slot + 1):
                            c1(h, s, way, slot + 1).start()
                if slot <= pairs:
                    for way in range(2):
                        if split(way, 1, slot - 1, pairs):
                            c2(h, s, way, 1, slot - 1).start()
                for i in range(pairs):
                    k = slot - 1 - i
                    if 1 <= k <= top:
                        for way in range(2):
                            if split(way, k, i, pairs):
                                c2(h, s, way, k, i).wait_recv()
                            if k < top and split(way, k + 1, i, pairs):
                                c2(h, s, way, k + 1, i).start()
        if slot < last:
            use_slot(slot - 1)
    use_slot(last)

    def e1(d):
        return pltpu.make_async_remote_copy(
            src_ref=give.at[plus(z, -d)],
            dst_ref=got.at[z],
            send_sem=e1_send.at[d],
            recv_sem=e1_recv.at[d],
            device_id={"shard_1": plus(z, -d)},
            device_id_type=MESH,
        )

    for a in range(n):
        for s in range(cap):
            at = s * hcells + (a % top) * n
            give[a, s] = acc[a // top, at : at + n, :].astype(BF16)
    for d in far:
        e1(d).start()
    got[z] = give[z]

    at_tok = lax.broadcasted_iota(jnp.int32, (8, 128), 0)
    at_row = lax.broadcasted_iota(jnp.int32, (8, 128), 1)
    whose = jnp.where(at_row < n * cap, at_row // cap, -1)
    coefs = jnp.zeros((8, 128), F32)
    for t, code in enumerate(codes_of(whose)):
        weight = jnp.where(ids[0][t] == whose, amount[0][t], 0.0) + jnp.where(
            ids[1][t] == whose, amount[1][t], 0.0
        )
        mine = (at_tok == t) & (code == (at_row % cap + 1).astype(F32))
        coefs = jnp.where(mine, weight, coefs)

    for d in far:
        e1(d).wait_recv()
    got32[...] = got[...].astype(F32).reshape(got32.shape)
    for b in range(n):
        mine = got32[pl.ds(b, n * cap, stride=n), :]
        pass_on[b] = mine.reshape(cap, n, 128).astype(BF16)

    def e2(b, src):
        return pltpu.make_async_remote_copy(
            src_ref=pass_on.at[b],
            dst_ref=back.at[src],
            send_sem=e2_send.at[b],
            recv_sem=e2_recv.at[src],
            device_id={"expert": y, "shard_0": b},
            device_id_type=MESH,
        )

    for b in range(n):
        here = (e == y) & (y == b)

        @pl.when(jnp.logical_not(here))
        def _(b=b):
            e2(b, e).start()

        @pl.when(here)
        def _(b=b):
            back[e] = pass_on[b]

    for src in range(n):

        @pl.when(jnp.logical_not((src == e) & (y == e)))
        def _(src=src):
            e2(0, src).wait_recv()

    low = lax.broadcasted_iota(jnp.int32, (1, 128), 1) < 64
    sums = [jnp.zeros((8, 128), F32) for _ in range(n // 2)]
    for src in range(n):
        value = back[src].astype(F32).reshape(n * cap, 128)
        for s in range(cap):
            at = src * cap + s
            coef = coefs[:, at : at + 1]
            for g in range(n // 2):
                a, b = 2 * g * cap + s, (2 * g + 1) * cap + s
                sums[g] = sums[g] + coef * jnp.where(low, value[a : a + 1, :], value[b : b + 1, :])
    for g in range(n // 2):
        out_ref[:, g * 128 : (g + 1) * 128] = sums[g][:tok_count, :].astype(BF16)

    for h in range(2):
        for d in range(1, n):
            a1(h, d).wait_send()
            a2(h, d).wait_send()
        for s in range(cap):
            for way in range(2):
                for k in range(1, top + 1):
                    for j in range(CHUNKS):
                        if split(way, k, j, CHUNKS):
                            a3(h, s, way, k, j).wait_send()
                    if in_line(s, way, k):
                        c1(h, s, way, k).wait_send()
                    for i in range(pairs):
                        if split(way, k, i, pairs):
                            c2(h, s, way, k, i).wait_send()
    for d in range(1, n):
        e1(d).wait_send()
    for b in range(n):

        @pl.when(jnp.logical_not((e == y) & (y == b)))
        def _(b=b):
            e2(b, e).wait_send()


def shards(n, tokens, expert_ids, gates, gate_proj, up_proj, down_proj_t):
    tok_count, feats = tokens.shape
    half = feats // 2
    hidden_units = gate_proj.shape[2]
    out_feats = down_proj_t.shape[1]
    cap = min(tok_count, 4 * tok_count // n)
    cells = n * n
    top = n // 2
    dma = pltpu.SemaphoreType.DMA
    vmem = pltpu.VMEM
    return pl.pallas_call(
        functools.partial(kernel, n, cap),
        out_shape=jax.ShapeDtypeStruct((tok_count, feats), BF16),
        in_specs=[pl.BlockSpec(memory_space=pl.ANY)] * 6,
        out_specs=pl.BlockSpec(memory_space=vmem),
        scratch_shapes=[
            vmem(tokens.shape, BF16),
            vmem((2, tok_count), jnp.int32),
            vmem((2, tok_count), F32),
            vmem((8, feats), F32),
            vmem((2, n, 8, half), BF16),
            vmem((2, n, cap, n, half), BF16),
            vmem((2, cap, n, n, n, half), BF16),
            vmem((2, cells, hidden_units), F32),
            vmem((2, cap, n, n, cells // 2, hidden_units), BF16),
            vmem((2, cap * cells // 2, 128), F32),
            vmem((n, cap, n, 128), BF16),
            vmem((n, cap, n, 128), BF16),
            vmem((n * cap * n, 128), F32),
            vmem((n, cap, n, 128), BF16),
            vmem((n, cap, n, 128), BF16),
            vmem(gate_proj.shape[1:], BF16),
            vmem(up_proj.shape[1:], BF16),
            vmem((2, out_feats, down_proj_t.shape[2]), BF16),
            dma((7,)),
            dma((2, n)), dma((2, n)),
            dma((2, n)), dma((2, n)),
            dma((2, cap, 2, top, CHUNKS)), dma((2, cap, 2, top, CHUNKS)),
            dma((2, cap, 2, top)), dma((2, cap, 2, top)),
            dma((2, cap, 2, top, n // 2)), dma((2, cap, 2, top, n // 2)),
            dma((n,)), dma((n,)),
            dma((n,)), dma((n,)),
        ],
        compiler_params=pltpu.CompilerParams(collective_id=0, has_side_effects=True),
        name="experts",
    )(tokens, expert_ids.T, gates.T, gate_proj[0], up_proj[0], down_proj_t[0])


def solution(mesh):
    n = mesh.shape["expert"]
    split = Mesh(mesh.devices.reshape(n, n, n), ("expert", "shard_0", "shard_1"))
    placed = (
        P(SHARD, "expert"),
        P(SHARD, None),
        P(SHARD, None),
        P("expert", None, SHARD),
        P("expert", None, SHARD),
        P("expert", SHARD, None),
    )
    return jax.shard_map(
        functools.partial(shards, n),
        mesh=split,
        in_specs=placed,
        out_specs=P(SHARD, "expert"),
        check_vma=False,
    )
```

```python
import functools

import jax
import jax.numpy as jnp
from jax import lax
from jax.experimental import pallas as pl
from jax.experimental.pallas import tpu as pltpu
from jax.sharding import Mesh
from jax.sharding import PartitionSpec as P

SHARD = ("shard_0", "shard_1")
MESH = pl.DeviceIdType.MESH
NARROW = ("shard_1", "shard_0")
WIDE = ("shard_0", "shard_1")
CHUNKS = 2
LEAPS = (0, 1, 2)
SPAN = 64
F32, BF16 = jnp.float32, jnp.bfloat16


def kernel(
    n, cap, tok_hbm, ids_hbm, gates_hbm, gate_hbm, up_hbm, down_hbm, out_ref,
    tok_v, ids_v, gates_v, stage, toks, sel, rows, part, hid, acc, give, got, got32, pass_on, back,
    gate_w, up_w, down_w,
    load_sem, a1_send, a1_recv, a2_send, a2_recv, a3_send, a3_recv,
    c1_send, c1_recv, c2_send, c2_recv, e1_send, e1_recv, e2_send, e2_recv,
):
    e = lax.axis_index("expert")
    y = lax.axis_index("shard_0")
    z = lax.axis_index("shard_1")
    nar = (z, y)
    wid = (y, z)
    top = n // 2
    cells = n * n
    hcells = cells // 2
    tok_count, feats = tok_v.shape
    half = feats // 2
    hidden_units = gate_w.shape[1]
    per = n // CHUNKS
    far = [d for k in range(top) for d in sorted({top - k, top + k}) if d < n]

    def plus(a, b):
        return lax.rem(a + b + n, n)

    small = [
        pltpu.make_async_copy(ids_hbm, ids_v, load_sem.at[0]),
        pltpu.make_async_copy(gates_hbm, gates_v, load_sem.at[1]),
        pltpu.make_async_copy(tok_hbm, tok_v, load_sem.at[2]),
    ]
    loads = [
        pltpu.make_async_copy(gate_hbm, gate_w, load_sem.at[3]),
        pltpu.make_async_copy(up_hbm, up_w, load_sem.at[4]),
        pltpu.make_async_copy(down_hbm, down_w.at[0], load_sem.at[5]),
        pltpu.make_async_copy(down_hbm, down_w.at[1], load_sem.at[6]),
    ]
    for copy in small:
        copy.start()
    barrier = pltpu.get_barrier_semaphore()
    for d in far:
        for axis, own in (("shard_1", z), ("shard_0", y), ("expert", e)):
            pl.semaphore_signal(
                barrier, inc=1, device_id={axis: plus(own, d)}, device_id_type=MESH
            )
    for copy in small:
        copy.wait()
    for copy in loads:
        copy.start()

    ids = [[ids_v[k : k + 1, t : t + 1] for t in range(tok_count)] for k in range(2)]
    amount = [[gates_v[k : k + 1, t : t + 1] for t in range(tok_count)] for k in range(2)]

    def codes_of(expert):
        run = jnp.zeros(expert.shape, F32)
        out = []
        for t in range(tok_count):
            hit = (ids[0][t] == expert) | (ids[1][t] == expert)
            out.append(jnp.where(hit, run + 1.0, 0.0))
            run = run + jnp.where(hit, 1.0, 0.0)
        return out

    sub = lax.broadcasted_iota(jnp.int32, (8, half), 0)
    lane = lax.broadcasted_iota(jnp.int32, (8, half), 1)
    held = half // SPAN
    expert = jnp.where(sub >= 6, (sub - 6) * held + lane // SPAN, -1)
    codes = codes_of(expert)
    stage[...] = jnp.zeros_like(stage)
    stage[0:tok_count, :] = tok_v[...].astype(F32)
    for h in range(2):
        here = (lane % SPAN) // 8 == nar[h]
        spare = jnp.zeros((8, half), F32)
        for t in range(tok_count):
            spare = jnp.where(here & (lane % 8 == t), codes[t], spare)
        toks[h, nar[h]] = (stage[:, h * half : (h + 1) * half] + spare).astype(BF16)

    pl.semaphore_wait(barrier, 3 * (n - 1))

    def a1(h, d):
        block = toks.at[h, nar[h]]
        return pltpu.make_async_remote_copy(
            src_ref=block,
            dst_ref=block,
            send_sem=a1_send.at[h, d],
            recv_sem=a1_recv.at[h, d],
            device_id={NARROW[h]: plus(nar[h], -d)},
            device_id_type=MESH,
        )

    for d in far:
        for h in range(2):
            a1(h, d).start()

    def a2(h, d):
        return pltpu.make_async_remote_copy(
            src_ref=sel.at[h, plus(e, -d)],
            dst_ref=rows.at[h, :, wid[h], d],
            send_sem=a2_send.at[h, d],
            recv_sem=a2_recv.at[h, d],
            device_id={"expert": plus(e, -d)},
            device_id_type=MESH,
        )

    m = held * cap * n
    row_of = lax.broadcasted_iota(jnp.int32, (m, half), 0)
    lane_of = lax.broadcasted_iota(jnp.int32, (m, half), 1)
    meets = ((lane_of % SPAN) // 8 == row_of % n) & (lane_of // SPAN == row_of // (cap * n))
    wanted = jnp.where(meets, ((row_of // n) % cap + 1).astype(F32), -1.0)
    for h in range(2):
        for d in far:
            a1(h, d).wait_recv()
        marks = jnp.zeros((8, half), F32)
        for b in range(n):
            marks = marks + toks[h, b].astype(F32)
        block = toks[h].reshape(8 * n, half)
        if 8 * n < SPAN:
            block = jnp.concatenate([block, jnp.zeros((SPAN - 8 * n, half), BF16)], axis=0)
        block = jnp.concatenate([block] * held, axis=0)
        pick = jnp.concatenate(
            [jnp.where(marks[6 + r : 7 + r, :] == wanted, 1.0, 0.0) for r in range(n // held)],
            axis=0,
        ).astype(BF16)
        found = jnp.dot(pick, block, preferred_element_type=F32)
        sel[h] = found.reshape(n, cap, n, half).astype(BF16)
        for d in range(1, n):
            a2(h, d).start()
        rows[h, :, wid[h], 0] = sel[h, e]

    def a3(h, s, way, k, j):
        step = 1 if way == 0 else -1
        base = k - 1 if s not in LEAPS else (0 if k <= 2 else 2)
        unit = rows.at[h, s, plus(wid[h], -step * base), pl.ds(j * per, per)]
        return pltpu.make_async_remote_copy(
            src_ref=unit,
            dst_ref=unit,
            send_sem=a3_send.at[h, s, way, k - 1, j],
            recv_sem=a3_recv.at[h, s, way, k - 1, j],
            device_id={WIDE[h]: plus(wid[h], step * (k - base))},
            device_id_type=MESH,
        )

    def split(way, k, j, count):
        return k < top or (j < count // 2) == (way == 0)

    for j in range(CHUNKS):
        for h in range(2):
            for d in range(j * per, (j + 1) * per):
                if d > 0:
                    a2(h, d).wait_recv()
        for s in range(cap):
            for h in range(2):
                for way in range(2):
                    for k in (2, 1) if s in LEAPS else (1,):
                        if k <= top and split(way, k, j, CHUNKS):
                            a3(h, s, way, k, j).start()

    def pass_rows(s, k):
        for j in range(CHUNKS):
            for h in range(2):
                for way in range(2):
                    if split(way, k, j, CHUNKS):
                        a3(h, s, way, k, j).wait_recv()
                    after = (k + 1,) if s not in LEAPS else ((4, 3) if k == 2 else ())
                    for later in after:
                        if later <= top and split(way, later, j, CHUNKS):
                            a3(h, s, way, later, j).start()

    order = [0]
    for d in range(1, top):
        order += [d, n - d]
    order.append(top)
    place = {d: p for p, d in enumerate(order)}

    def c1(h, s, d):
        send, to = (0, -d) if d != top else ((top - 1, -1) if s % 2 == 0 else ((1 - top) % n, 1))
        return pltpu.make_async_remote_copy(
            src_ref=hid.at[h, s, wid[h], place[send]],
            dst_ref=hid.at[h, s, wid[h], place[d]],
            send_sem=c1_send.at[h, s, d],
            recv_sem=c1_recv.at[h, s, d],
            device_id={NARROW[h]: plus(nar[h], to)},
            device_id_type=MESH,
        )

    def c2(h, s, way, k, i):
        step = 1 if way == 0 else -1
        unit = hid.at[h, s, plus(wid[h], -step * (k - 1)), pl.ds(2 * i, 2)]
        return pltpu.make_async_remote_copy(
            src_ref=unit,
            dst_ref=unit,
            send_sem=c2_send.at[h, s, way, k - 1, i],
            recv_sem=c2_recv.at[h, s, way, k - 1, i],
            device_id={WIDE[h]: plus(wid[h], step)},
            device_id_type=MESH,
        )

    def project(s):
        sums = []
        for h in range(2):
            total = jnp.zeros((cells, 2 * hidden_units), F32)
            for d in range(n):
                at = pl.multiple_of(plus(e, d) * (2 * half) + h * half, half)
                lhs = rows[h, s, :, d].reshape(cells, half)
                rhs = jnp.concatenate(
                    [gate_w[pl.ds(at, half), :], up_w[pl.ds(at, half), :]], axis=1
                )
                total = total + jnp.dot(lhs, rhs, preferred_element_type=F32)
            sums.append(total)
        for c in range(2):
            part[c] = sums[0][:, c * hidden_units : (c + 1) * hidden_units]
        gated, up = (
            jnp.concatenate([part[c, pl.ds(b, n, stride=n), :] for b in range(n)], axis=0)
            + sums[1][:, c * hidden_units : (c + 1) * hidden_units]
            for c in range(2)
        )
        hidden = ((gated / (1.0 + jnp.exp(-gated))) * up).astype(BF16)
        for h in range(2):
            hid[h, s, wid[h], 0] = hidden[h * hcells : (h + 1) * hcells, :]

    def begin(s):
        project(s)
        for k in range(top - 1, 0, -1):
            for d in (k, n - k):
                for h in range(2):
                    c1(h, s, d).start()
        if top == 1:
            for h in range(2):
                c1(h, s, top).start()

    slow = [s for s in range(cap) if s not in LEAPS]
    quick = [s for s in range(cap) if s in LEAPS]
    for k in range(1, top + 1):
        for s in slow if k < top else ():
            pass_rows(s, k)
        if k == 2 or k == top == 1:
            for s in quick:
                for q in range(1, min(top, 2) + 1):
                    pass_rows(s, q)
        if k == min(3, top):
            for copy in loads:
                copy.wait()
            for s in quick:
                for q in range(3, top + 1):
                    pass_rows(s, q)
                begin(s)
    for s in slow:
        pass_rows(s, top)
        begin(s)

    acc[...] = jnp.zeros_like(acc)
    pairs = n // 2

    def use(h, src, i):
        lhs, rhs = [], []
        for p in (2 * i, 2 * i + 1):
            other = plus(nar[h], order[p])
            unit = src * n + other if h == 0 else other * n + src
            at = pl.multiple_of(unit * hidden_units, hidden_units)
            lhs.append(hid[h, :, src, p].reshape(cap * hcells, hidden_units))
            rhs.append(down_w[:, :, pl.ds(at, hidden_units)].reshape(128, hidden_units))
        acc[h] += lax.dot_general(
            jnp.concatenate(lhs, axis=1),
            jnp.concatenate(rhs, axis=1),
            (((1,), (1,)), ((), ())),
            preferred_element_type=F32,
        )

    early = pairs - 1

    def use_step(t):
        for h in range(2):
            for i in range(pairs):
                k = t if i < early else t - 1
                if k == 0:
                    use(h, wid[h], i)
                elif 1 <= k < top:
                    use(h, plus(wid[h], -k), i)
                    use(h, plus(wid[h], k), i)
                elif k == top:
                    use(h, plus(wid[h], k), i)

    def launch(h, s, i):
        for way in range(2):
            if split(way, 1, i, pairs):
                c2(h, s, way, 1, i).start()

    def pass_hidden(h, s, k, i):
        for way in range(2):
            if split(way, k, i, pairs):
                c2(h, s, way, k, i).wait_recv()
            if k < top and split(way, k + 1, i, pairs):
                c2(h, s, way, k + 1, i).start()

    for s in range(cap):
        for h in range(2):
            for p in range(1, n - 1):
                c1(h, s, order[p]).wait_recv()
                if p % 2 == 1:
                    launch(h, s, p // 2)
                if top > 1 and order[p] == (top - 1 if s % 2 == 0 else n - top + 1):
                    c1(h, s, top).start()
    for t in range(1, top + 2):
        if t == top + 1:
            use_step(top)
        for s in range(cap):
            for h in range(2):
                for i in range(early if t <= top else 0):
                    pass_hidden(h, s, t, i)
                if t == 1:
                    c1(h, s, top).wait_recv()
                    launch(h, s, pairs - 1)
                else:
                    pass_hidden(h, s, t - 1, pairs - 1)
        if t <= top:
            use_step(t - 1)
    use_step(top + 1)

    def e1(d):
        return pltpu.make_async_remote_copy(
            src_ref=give.at[plus(z, -d)],
            dst_ref=got.at[z],
            send_sem=e1_send.at[d],
            recv_sem=e1_recv.at[d],
            device_id={"shard_1": plus(z, -d)},
            device_id_type=MESH,
        )

    for a in range(n):
        for s in range(cap):
            at = s * hcells + (a % top) * n
            give[a, s] = acc[a // top, at : at + n, :].astype(BF16)
    for d in far:
        e1(d).start()
    got[z] = give[z]

    at_tok = lax.broadcasted_iota(jnp.int32, (8, 128), 0)
    at_row = lax.broadcasted_iota(jnp.int32, (8, 128), 1)
    whose = jnp.where(at_row < n * cap, at_row // cap, -1)
    coefs = jnp.zeros((8, 128), F32)
    for t, code in enumerate(codes_of(whose)):
        weight = jnp.where(ids[0][t] == whose, amount[0][t], 0.0) + jnp.where(
            ids[1][t] == whose, amount[1][t], 0.0
        )
        mine = (at_tok == t) & (code == (at_row % cap + 1).astype(F32))
        coefs = jnp.where(mine, weight, coefs)

    for d in far:
        e1(d).wait_recv()
    got32[...] = got[...].astype(F32).reshape(got32.shape)
    for b in range(n):
        mine = got32[pl.ds(b, n * cap, stride=n), :]
        pass_on[b] = mine.reshape(cap, n, 128).astype(BF16)

    def e2(b, src):
        return pltpu.make_async_remote_copy(
            src_ref=pass_on.at[b],
            dst_ref=back.at[src],
            send_sem=e2_send.at[b],
            recv_sem=e2_recv.at[src],
            device_id={"expert": y, "shard_0": b},
            device_id_type=MESH,
        )

    for b in range(n):
        here = (e == y) & (y == b)

        @pl.when(jnp.logical_not(here))
        def _(b=b):
            e2(b, e).start()

        @pl.when(here)
        def _(b=b):
            back[e] = pass_on[b]

    for src in range(n):

        @pl.when(jnp.logical_not((src == e) & (y == e)))
        def _(src=src):
            e2(0, src).wait_recv()

    low = lax.broadcasted_iota(jnp.int32, (1, 128), 1) < 64
    sums = [jnp.zeros((8, 128), F32) for _ in range(n // 2)]
    for src in range(n):
        value = back[src].astype(F32).reshape(n * cap, 128)
        for s in range(cap):
            at = src * cap + s
            coef = coefs[:, at : at + 1]
            for g in range(n // 2):
                a, b = 2 * g * cap + s, (2 * g + 1) * cap + s
                sums[g] = sums[g] + coef * jnp.where(low, value[a : a + 1, :], value[b : b + 1, :])
    for g in range(n // 2):
        out_ref[:, g * 128 : (g + 1) * 128] = sums[g][:tok_count, :].astype(BF16)

    for h in range(2):
        for d in range(1, n):
            a1(h, d).wait_send()
            a2(h, d).wait_send()
        for s in range(cap):
            for d in range(1, n):
                c1(h, s, d).wait_send()
            for way in range(2):
                for k in range(1, top + 1):
                    for j in range(CHUNKS):
                        if split(way, k, j, CHUNKS):
                            a3(h, s, way, k, j).wait_send()
                    for i in range(pairs):
                        if split(way, k, i, pairs):
                            c2(h, s, way, k, i).wait_send()
    for d in range(1, n):
        e1(d).wait_send()
    for b in range(n):

        @pl.when(jnp.logical_not((e == y) & (y == b)))
        def _(b=b):
            e2(b, e).wait_send()


def shards(n, tokens, expert_ids, gates, gate_proj, up_proj, down_proj_t):
    tok_count, feats = tokens.shape
    half = feats // 2
    hidden_units = gate_proj.shape[2]
    out_feats = down_proj_t.shape[1]
    cap = min(tok_count, 4 * tok_count // n)
    cells = n * n
    top = n // 2
    dma = pltpu.SemaphoreType.DMA
    vmem = pltpu.VMEM
    return pl.pallas_call(
        functools.partial(kernel, n, cap),
        out_shape=jax.ShapeDtypeStruct((tok_count, feats), BF16),
        in_specs=[pl.BlockSpec(memory_space=pl.ANY)] * 6,
        out_specs=pl.BlockSpec(memory_space=vmem),
        scratch_shapes=[
            vmem(tokens.shape, BF16),
            vmem((2, tok_count), jnp.int32),
            vmem((2, tok_count), F32),
            vmem((8, feats), F32),
            vmem((2, n, 8, half), BF16),
            vmem((2, n, cap, n, half), BF16),
            vmem((2, cap, n, n, n, half), BF16),
            vmem((2, cells, hidden_units), F32),
            vmem((2, cap, n, n, cells // 2, hidden_units), BF16),
            vmem((2, cap * cells // 2, 128), F32),
            vmem((n, cap, n, 128), BF16),
            vmem((n, cap, n, 128), BF16),
            vmem((n * cap * n, 128), F32),
            vmem((n, cap, n, 128), BF16),
            vmem((n, cap, n, 128), BF16),
            vmem(gate_proj.shape[1:], BF16),
            vmem(up_proj.shape[1:], BF16),
            vmem((2, out_feats, down_proj_t.shape[2]), BF16),
            dma((7,)),
            dma((2, n)), dma((2, n)),
            dma((2, n)), dma((2, n)),
            dma((2, cap, 2, top, CHUNKS)), dma((2, cap, 2, top, CHUNKS)),
            dma((2, cap, n)), dma((2, cap, n)),
            dma((2, cap, 2, top, n // 2)), dma((2, cap, 2, top, n // 2)),
            dma((n,)), dma((n,)),
            dma((n,)), dma((n,)),
        ],
        compiler_params=pltpu.CompilerParams(collective_id=0, has_side_effects=True),
        name="experts",
    )(tokens, expert_ids.T, gates.T, gate_proj[0], up_proj[0], down_proj_t[0])


def solution(mesh):
    n = mesh.shape["expert"]
    split = Mesh(mesh.devices.reshape(n, n, n), ("expert", "shard_0", "shard_1"))
    placed = (
        P(SHARD, "expert"),
        P(SHARD, None),
        P(SHARD, None),
        P("expert", None, SHARD),
        P("expert", None, SHARD),
        P("expert", SHARD, None),
    )
    return jax.shard_map(
        functools.partial(shards, n),
        mesh=split,
        in_specs=placed,
        out_specs=P(SHARD, "expert"),
        check_vma=False,
    )
```

```python
import functools

import jax
import jax.numpy as jnp
from jax import lax
from jax.experimental import pallas as pl
from jax.experimental.pallas import tpu as pltpu
from jax.sharding import Mesh
from jax.sharding import PartitionSpec as P

SHARD = ("shard_0", "shard_1")
MESH = pl.DeviceIdType.MESH
NARROW = ("shard_1", "shard_0")
WIDE = ("shard_0", "shard_1")
CHUNKS = 2
LEAPS = (0, 1, 2)
SPAN = 64
F32, BF16 = jnp.float32, jnp.bfloat16


def kernel(
    n, cap, tok_hbm, ids_hbm, gates_hbm, gate_hbm, up_hbm, down_hbm, out_ref,
    tok_v, ids_v, gates_v, stage, toks, sel, rows, part, hid, acc, give, got, got32, pass_on, back,
    gate_w, up_w, down_w,
    load_sem, a1_send, a1_recv, a2_send, a2_recv, a3_send, a3_recv,
    c1_send, c1_recv, c2_send, c2_recv, e1_send, e1_recv, e2_send, e2_recv,
):
    e = lax.axis_index("expert")
    y = lax.axis_index("shard_0")
    z = lax.axis_index("shard_1")
    nar = (z, y)
    wid = (y, z)
    top = n // 2
    cells = n * n
    hcells = cells // 2
    tok_count, feats = tok_v.shape
    half = feats // 2
    hidden_units = gate_w.shape[1]
    per = n // CHUNKS
    far = [d for k in range(top) for d in sorted({top - k, top + k}) if d < n]

    def plus(a, b):
        return lax.rem(a + b + n, n)

    small = [
        pltpu.make_async_copy(ids_hbm, ids_v, load_sem.at[0]),
        pltpu.make_async_copy(gates_hbm, gates_v, load_sem.at[1]),
        pltpu.make_async_copy(tok_hbm, tok_v, load_sem.at[2]),
    ]
    loads = [
        pltpu.make_async_copy(gate_hbm, gate_w, load_sem.at[3]),
        pltpu.make_async_copy(up_hbm, up_w, load_sem.at[4]),
        pltpu.make_async_copy(down_hbm, down_w.at[0], load_sem.at[5]),
        pltpu.make_async_copy(down_hbm, down_w.at[1], load_sem.at[6]),
    ]
    for copy in small:
        copy.start()
    barrier = pltpu.get_barrier_semaphore()
    for d in far:
        for axis, own in (("shard_1", z), ("shard_0", y), ("expert", e)):
            pl.semaphore_signal(
                barrier, inc=1, device_id={axis: plus(own, d)}, device_id_type=MESH
            )
    for copy in small:
        copy.wait()
    for copy in loads:
        copy.start()

    ids = [[ids_v[k : k + 1, t : t + 1] for t in range(tok_count)] for k in range(2)]
    amount = [[gates_v[k : k + 1, t : t + 1] for t in range(tok_count)] for k in range(2)]

    def codes_of(expert):
        run = jnp.zeros(expert.shape, F32)
        out = []
        for t in range(tok_count):
            hit = (ids[0][t] == expert) | (ids[1][t] == expert)
            out.append(jnp.where(hit, run + 1.0, 0.0))
            run = run + jnp.where(hit, 1.0, 0.0)
        return out

    sub = lax.broadcasted_iota(jnp.int32, (8, half), 0)
    lane = lax.broadcasted_iota(jnp.int32, (8, half), 1)
    held = half // SPAN
    expert = jnp.where(sub >= 6, (sub - 6) * held + lane // SPAN, -1)
    codes = codes_of(expert)
    stage[...] = jnp.zeros_like(stage)
    stage[0:tok_count, :] = tok_v[...].astype(F32)
    for h in range(2):
        here = (lane % SPAN) // 8 == nar[h]
        spare = jnp.zeros((8, half), F32)
        for t in range(tok_count):
            spare = jnp.where(here & (lane % 8 == t), codes[t], spare)
        toks[h, nar[h]] = (stage[:, h * half : (h + 1) * half] + spare).astype(BF16)

    pl.semaphore_wait(barrier, 3 * (n - 1))

    def bytes_of(ref, sem):
        return pltpu.make_async_copy(ref, ref, sem).wait()

    def a1(h, d):
        block = toks.at[h, nar[h]]
        return pltpu.make_async_remote_copy(
            src_ref=block,
            dst_ref=block,
            send_sem=a1_send.at[h],
            recv_sem=a1_recv.at[h],
            device_id={NARROW[h]: plus(nar[h], -d)},
            device_id_type=MESH,
        )

    for d in far:
        for h in range(2):
            a1(h, d).start()

    def a2(h, d):
        return pltpu.make_async_remote_copy(
            src_ref=sel.at[h, plus(e, -d)],
            dst_ref=rows.at[h, :, wid[h], d],
            send_sem=a2_send.at[h],
            recv_sem=a2_recv.at[h, d // per],
            device_id={"expert": plus(e, -d)},
            device_id_type=MESH,
        )

    m = held * cap * n
    row_of = lax.broadcasted_iota(jnp.int32, (m, half), 0)
    lane_of = lax.broadcasted_iota(jnp.int32, (m, half), 1)
    meets = ((lane_of % SPAN) // 8 == row_of % n) & (lane_of // SPAN == row_of // (cap * n))
    wanted = jnp.where(meets, ((row_of // n) % cap + 1).astype(F32), -1.0)
    for h in range(2):
        bytes_of(toks.at[h, pl.ds(0, n - 1)], a1_recv.at[h])
        marks = jnp.zeros((8, half), F32)
        for b in range(n):
            marks = marks + toks[h, b].astype(F32)
        block = toks[h].reshape(8 * n, half)
        if 8 * n < SPAN:
            block = jnp.concatenate([block, jnp.zeros((SPAN - 8 * n, half), BF16)], axis=0)
        block = jnp.concatenate([block] * held, axis=0)
        pick = jnp.concatenate(
            [jnp.where(marks[6 + r : 7 + r, :] == wanted, 1.0, 0.0) for r in range(n // held)],
            axis=0,
        ).astype(BF16)
        found = jnp.dot(pick, block, preferred_element_type=F32)
        sel[h] = found.reshape(n, cap, n, half).astype(BF16)
        for d in range(1, n):
            a2(h, d).start()
        rows[h, :, wid[h], 0] = sel[h, e]

    def a3(h, s, way, k, j):
        step = 1 if way == 0 else -1
        base = k - 1 if s not in LEAPS else (0 if k <= 2 else 2)
        unit = rows.at[h, s, plus(wid[h], -step * base), pl.ds(j * per, per)]
        return pltpu.make_async_remote_copy(
            src_ref=unit,
            dst_ref=unit,
            send_sem=a3_send.at[h, s],
            recv_sem=a3_recv.at[h, s, way, k - 1, j],
            device_id={WIDE[h]: plus(wid[h], step * (k - base))},
            device_id_type=MESH,
        )

    def split(way, k, j, count):
        return k < top or (j < count // 2) == (way == 0)

    for j in range(CHUNKS):
        for h in range(2):
            count = per if j > 0 else per - 1
            if count > 0:
                bytes_of(sel.at[h, pl.ds(0, count)], a2_recv.at[h, j])
        for s in range(cap):
            for h in range(2):
                for way in range(2):
                    for k in (2, 1) if s in LEAPS else (1,):
                        if k <= top and split(way, k, j, CHUNKS):
                            a3(h, s, way, k, j).start()

    def pass_rows(s, k):
        for j in range(CHUNKS):
            for h in range(2):
                for way in range(2):
                    if split(way, k, j, CHUNKS):
                        a3(h, s, way, k, j).wait_recv()
                    after = (k + 1,) if s not in LEAPS else ((4, 3) if k == 2 else ())
                    for later in after:
                        if later <= top and split(way, later, j, CHUNKS):
                            a3(h, s, way, later, j).start()

    order = [0]
    for d in range(1, top):
        order += [d, n - d]
    order.append(top)
    place = {d: p for p, d in enumerate(order)}

    def c1(h, s, d):
        send, to = (0, -d) if d != top else ((top - 1, -1) if s % 2 == 0 else ((1 - top) % n, 1))
        return pltpu.make_async_remote_copy(
            src_ref=hid.at[h, s, wid[h], place[send]],
            dst_ref=hid.at[h, s, wid[h], place[d]],
            send_sem=c1_send.at[h, s],
            recv_sem=c1_recv.at[h, s, d],
            device_id={NARROW[h]: plus(nar[h], to)},
            device_id_type=MESH,
        )

    def c2(h, s, way, k, i):
        step = 1 if way == 0 else -1
        unit = hid.at[h, s, plus(wid[h], -step * (k - 1)), pl.ds(2 * i, 2)]
        return pltpu.make_async_remote_copy(
            src_ref=unit,
            dst_ref=unit,
            send_sem=c2_send.at[h, s],
            recv_sem=c2_recv.at[h, s, way, k - 1, i],
            device_id={WIDE[h]: plus(wid[h], step)},
            device_id_type=MESH,
        )

    def project(s):
        sums = []
        for h in range(2):
            total = jnp.zeros((cells, 2 * hidden_units), F32)
            for d in range(n):
                at = pl.multiple_of(plus(e, d) * (2 * half) + h * half, half)
                lhs = rows[h, s, :, d].reshape(cells, half)
                rhs = jnp.concatenate(
                    [gate_w[pl.ds(at, half), :], up_w[pl.ds(at, half), :]], axis=1
                )
                total = total + jnp.dot(lhs, rhs, preferred_element_type=F32)
            sums.append(total)
        for c in range(2):
            part[c] = sums[0][:, c * hidden_units : (c + 1) * hidden_units]
        gated, up = (
            jnp.concatenate([part[c, pl.ds(b, n, stride=n), :] for b in range(n)], axis=0)
            + sums[1][:, c * hidden_units : (c + 1) * hidden_units]
            for c in range(2)
        )
        hidden = ((gated / (1.0 + jnp.exp(-gated))) * up).astype(BF16)
        for h in range(2):
            hid[h, s, wid[h], 0] = hidden[h * hcells : (h + 1) * hcells, :]

    def begin(s):
        project(s)
        for k in range(top - 1, 0, -1):
            for d in (k, n - k):
                for h in range(2):
                    c1(h, s, d).start()
        if top == 1:
            for h in range(2):
                c1(h, s, top).start()

    slow = [s for s in range(cap) if s not in LEAPS]
    quick = [s for s in range(cap) if s in LEAPS]
    for k in range(1, top + 1):
        for s in slow if k < top else ():
            pass_rows(s, k)
        if k == 2 or k == top == 1:
            for s in quick:
                for q in range(1, min(top, 2) + 1):
                    pass_rows(s, q)
        if k == min(3, top):
            for copy in loads:
                copy.wait()
            for s in quick:
                for q in range(3, top + 1):
                    pass_rows(s, q)
                begin(s)
    for s in slow:
        pass_rows(s, top)
        begin(s)

    acc[...] = jnp.zeros_like(acc)
    pairs = n // 2

    def use(h, src, i):
        lhs, rhs = [], []
        for p in (2 * i, 2 * i + 1):
            other = plus(nar[h], order[p])
            unit = src * n + other if h == 0 else other * n + src
            at = pl.multiple_of(unit * hidden_units, hidden_units)
            lhs.append(hid[h, :, src, p].reshape(cap * hcells, hidden_units))
            rhs.append(down_w[:, :, pl.ds(at, hidden_units)].reshape(128, hidden_units))
        acc[h] += lax.dot_general(
            jnp.concatenate(lhs, axis=1),
            jnp.concatenate(rhs, axis=1),
            (((1,), (1,)), ((), ())),
            preferred_element_type=F32,
        )

    early = pairs - 1

    def use_step(t):
        for h in range(2):
            for i in range(pairs):
                k = t if i < early else t - 1
                if k == 0:
                    use(h, wid[h], i)
                elif 1 <= k < top:
                    use(h, plus(wid[h], -k), i)
                    use(h, plus(wid[h], k), i)
                elif k == top:
                    use(h, plus(wid[h], k), i)

    def launch(h, s, i):
        for way in range(2):
            if split(way, 1, i, pairs):
                c2(h, s, way, 1, i).start()

    def pass_hidden(h, s, k, i):
        for way in range(2):
            if split(way, k, i, pairs):
                c2(h, s, way, k, i).wait_recv()
            if k < top and split(way, k + 1, i, pairs):
                c2(h, s, way, k + 1, i).start()

    for s in range(cap):
        for h in range(2):
            for p in range(1, n - 1):
                c1(h, s, order[p]).wait_recv()
                if p % 2 == 1:
                    launch(h, s, p // 2)
                if top > 1 and order[p] == (top - 1 if s % 2 == 0 else n - top + 1):
                    c1(h, s, top).start()
    for t in range(1, top + 2):
        if t == top + 1:
            use_step(top)
        for s in range(cap):
            for h in range(2):
                for i in range(early if t <= top else 0):
                    pass_hidden(h, s, t, i)
                if t == 1:
                    c1(h, s, top).wait_recv()
                    launch(h, s, pairs - 1)
                else:
                    pass_hidden(h, s, t - 1, pairs - 1)
        if t <= top:
            use_step(t - 1)
    use_step(top + 1)

    def e1(d):
        return pltpu.make_async_remote_copy(
            src_ref=give.at[plus(z, -d)],
            dst_ref=got.at[z],
            send_sem=e1_send,
            recv_sem=e1_recv,
            device_id={"shard_1": plus(z, -d)},
            device_id_type=MESH,
        )

    for a in range(n):
        for s in range(cap):
            at = s * hcells + (a % top) * n
            give[a, s] = acc[a // top, at : at + n, :].astype(BF16)
    for d in far:
        e1(d).start()
    got[z] = give[z]

    at_tok = lax.broadcasted_iota(jnp.int32, (8, 128), 0)
    at_row = lax.broadcasted_iota(jnp.int32, (8, 128), 1)
    whose = jnp.where(at_row < n * cap, at_row // cap, -1)
    coefs = jnp.zeros((8, 128), F32)
    for t, code in enumerate(codes_of(whose)):
        weight = jnp.where(ids[0][t] == whose, amount[0][t], 0.0) + jnp.where(
            ids[1][t] == whose, amount[1][t], 0.0
        )
        mine = (at_tok == t) & (code == (at_row % cap + 1).astype(F32))
        coefs = jnp.where(mine, weight, coefs)

    for h in range(2):
        bytes_of(toks.at[h, pl.ds(0, n - 1)], a1_send.at[h])
        bytes_of(sel.at[h, pl.ds(0, n - 1)], a2_send.at[h])
        for s in range(cap):
            bytes_of(rows.at[h, s, pl.ds(0, n - 1)], a3_send.at[h, s])
            bytes_of(hid.at[h, s, 0, pl.ds(0, n - 1)], c1_send.at[h, s])
            bytes_of(hid.at[h, s, pl.ds(0, n - 1)], c2_send.at[h, s])
    bytes_of(give.at[pl.ds(0, n - 1)], e1_recv)
    got32[...] = got[...].astype(F32).reshape(got32.shape)
    for b in range(n):
        mine = got32[pl.ds(b, n * cap, stride=n), :]
        pass_on[b] = mine.reshape(cap, n, 128).astype(BF16)

    def e2(b, src):
        return pltpu.make_async_remote_copy(
            src_ref=pass_on.at[b],
            dst_ref=back.at[src],
            send_sem=e2_send,
            recv_sem=e2_recv,
            device_id={"expert": y, "shard_0": b},
            device_id_type=MESH,
        )

    for b in range(n):
        here = (e == y) & (y == b)

        @pl.when(jnp.logical_not(here))
        def _(b=b):
            e2(b, e).start()

        @pl.when(here)
        def _(b=b):
            back[e] = pass_on[b]

    @pl.when(e == y)
    def _():
        bytes_of(back.at[pl.ds(0, n - 1)], e2_recv)

    @pl.when(e != y)
    def _():
        bytes_of(back, e2_recv)

    low = lax.broadcasted_iota(jnp.int32, (1, 128), 1) < 64
    sums = [jnp.zeros((8, 128), F32) for _ in range(n // 2)]
    for src in range(n):
        value = back[src].astype(F32).reshape(n * cap, 128)
        for s in range(cap):
            at = src * cap + s
            coef = coefs[:, at : at + 1]
            for g in range(n // 2):
                a, b = 2 * g * cap + s, (2 * g + 1) * cap + s
                sums[g] = sums[g] + coef * jnp.where(low, value[a : a + 1, :], value[b : b + 1, :])
    for g in range(n // 2):
        out_ref[:, g * 128 : (g + 1) * 128] = sums[g][:tok_count, :].astype(BF16)

    bytes_of(give.at[pl.ds(0, n - 1)], e1_send)

    @pl.when(e == y)
    def _():
        bytes_of(pass_on.at[pl.ds(0, n - 1)], e2_send)

    @pl.when(e != y)
    def _():
        bytes_of(pass_on, e2_send)


def shards(n, tokens, expert_ids, gates, gate_proj, up_proj, down_proj_t):
    tok_count, feats = tokens.shape
    half = feats // 2
    hidden_units = gate_proj.shape[2]
    out_feats = down_proj_t.shape[1]
    cap = min(tok_count, 4 * tok_count // n)
    cells = n * n
    top = n // 2
    dma = pltpu.SemaphoreType.DMA
    vmem = pltpu.VMEM
    return pl.pallas_call(
        functools.partial(kernel, n, cap),
        out_shape=jax.ShapeDtypeStruct((tok_count, feats), BF16),
        in_specs=[pl.BlockSpec(memory_space=pl.ANY)] * 6,
        out_specs=pl.BlockSpec(memory_space=vmem),
        scratch_shapes=[
            vmem(tokens.shape, BF16),
            vmem((2, tok_count), jnp.int32),
            vmem((2, tok_count), F32),
            vmem((8, feats), F32),
            vmem((2, n, 8, half), BF16),
            vmem((2, n, cap, n, half), BF16),
            vmem((2, cap, n, n, n, half), BF16),
            vmem((2, cells, hidden_units), F32),
            vmem((2, cap, n, n, cells // 2, hidden_units), BF16),
            vmem((2, cap * cells // 2, 128), F32),
            vmem((n, cap, n, 128), BF16),
            vmem((n, cap, n, 128), BF16),
            vmem((n * cap * n, 128), F32),
            vmem((n, cap, n, 128), BF16),
            vmem((n, cap, n, 128), BF16),
            vmem(gate_proj.shape[1:], BF16),
            vmem(up_proj.shape[1:], BF16),
            vmem((2, out_feats, down_proj_t.shape[2]), BF16),
            dma((7,)),
            dma((2,)), dma((2,)),
            dma((2,)), dma((2, CHUNKS)),
            dma((2, cap)), dma((2, cap, 2, top, CHUNKS)),
            dma((2, cap)), dma((2, cap, n)),
            dma((2, cap)), dma((2, cap, 2, top, n // 2)),
            dma, dma,
            dma, dma,
        ],
        compiler_params=pltpu.CompilerParams(collective_id=0, has_side_effects=True),
        name="experts",
    )(tokens, expert_ids.T, gates.T, gate_proj[0], up_proj[0], down_proj_t[0])


def solution(mesh):
    n = mesh.shape["expert"]
    split = Mesh(mesh.devices.reshape(n, n, n), ("expert", "shard_0", "shard_1"))
    placed = (
        P(SHARD, "expert"),
        P(SHARD, None),
        P(SHARD, None),
        P("expert", None, SHARD),
        P("expert", None, SHARD),
        P("expert", SHARD, None),
    )
    return jax.shard_map(
        functools.partial(shards, n),
        mesh=split,
        in_specs=placed,
        out_specs=P(SHARD, "expert"),
        check_vma=False,
    )
```

```python
import functools

import jax
import jax.numpy as jnp
from jax import lax
from jax.experimental import pallas as pl
from jax.experimental.pallas import tpu as pltpu
from jax.sharding import Mesh
from jax.sharding import PartitionSpec as P

SHARD = ("shard_0", "shard_1")
MESH = pl.DeviceIdType.MESH
NARROW = ("shard_1", "shard_0")
WIDE = ("shard_0", "shard_1")
CHUNKS = 2
SPAN = 64
F32, BF16 = jnp.float32, jnp.bfloat16


def kernel(
    n, cap, tok_hbm, ids_hbm, gates_hbm, gate_hbm, up_hbm, down_hbm, out_ref,
    tok_v, ids_v, gates_v, stage, toks, sel, rows, part, hid, acc, give, got, got32, pass_on, back,
    gate_w, up_w, down_w,
    load_sem, a1_send, a1_recv, a2_send, a2_recv, a3_send, a3_recv,
    c1_send, c1_recv, c2_send, c2_recv, e1_send, e1_recv, e2_send, e2_recv,
):
    e = lax.axis_index("expert")
    y = lax.axis_index("shard_0")
    z = lax.axis_index("shard_1")
    nar = (z, y)
    wid = (y, z)
    top = n // 2
    cells = n * n
    hcells = cells // 2
    tok_count, feats = tok_v.shape
    half = feats // 2
    hidden_units = gate_w.shape[1]
    per = n // CHUNKS
    far = [d for k in range(top) for d in sorted({top - k, top + k}) if d < n]

    def plus(a, b):
        return lax.rem(a + b + n, n)

    small = [
        pltpu.make_async_copy(ids_hbm, ids_v, load_sem.at[0]),
        pltpu.make_async_copy(gates_hbm, gates_v, load_sem.at[1]),
        pltpu.make_async_copy(tok_hbm, tok_v, load_sem.at[2]),
    ]
    loads = [
        pltpu.make_async_copy(gate_hbm, gate_w, load_sem.at[3]),
        pltpu.make_async_copy(up_hbm, up_w, load_sem.at[4]),
        pltpu.make_async_copy(down_hbm, down_w.at[0], load_sem.at[5]),
        pltpu.make_async_copy(down_hbm, down_w.at[1], load_sem.at[6]),
    ]
    for copy in small:
        copy.start()
    barrier = pltpu.get_barrier_semaphore()
    for d in far:
        for axis, own in (("shard_1", z), ("shard_0", y), ("expert", e)):
            pl.semaphore_signal(
                barrier, inc=1, device_id={axis: plus(own, d)}, device_id_type=MESH
            )
    for copy in small:
        copy.wait()
    for copy in loads:
        copy.start()

    ids = [[ids_v[k : k + 1, t : t + 1] for t in range(tok_count)] for k in range(2)]
    amount = [[gates_v[k : k + 1, t : t + 1] for t in range(tok_count)] for k in range(2)]

    def codes_of(expert):
        run = jnp.zeros(expert.shape, F32)
        out = []
        for t in range(tok_count):
            hit = (ids[0][t] == expert) | (ids[1][t] == expert)
            out.append(jnp.where(hit, run + 1.0, 0.0))
            run = run + jnp.where(hit, 1.0, 0.0)
        return out

    sub = lax.broadcasted_iota(jnp.int32, (8, half), 0)
    lane = lax.broadcasted_iota(jnp.int32, (8, half), 1)
    held = half // SPAN
    expert = jnp.where(sub >= 6, (sub - 6) * held + lane // SPAN, -1)
    codes = codes_of(expert)
    stage[...] = jnp.zeros_like(stage)
    stage[0:tok_count, :] = tok_v[...].astype(F32)
    for h in range(2):
        here = (lane % SPAN) // 8 == nar[h]
        spare = jnp.zeros((8, half), F32)
        for t in range(tok_count):
            spare = jnp.where(here & (lane % 8 == t), codes[t], spare)
        toks[h, nar[h]] = (stage[:, h * half : (h + 1) * half] + spare).astype(BF16)

    pl.semaphore_wait(barrier, 3 * (n - 1))

    def bytes_of(ref, sem):
        return pltpu.make_async_copy(ref, ref, sem).wait()

    def a1(h, d):
        block = toks.at[h, nar[h]]
        return pltpu.make_async_remote_copy(
            src_ref=block,
            dst_ref=block,
            send_sem=a1_send.at[h],
            recv_sem=a1_recv.at[h],
            device_id={NARROW[h]: plus(nar[h], -d)},
            device_id_type=MESH,
        )

    for d in far:
        for h in range(2):
            a1(h, d).start()

    def a2(h, d):
        return pltpu.make_async_remote_copy(
            src_ref=sel.at[h, plus(e, -d)],
            dst_ref=rows.at[h, :, wid[h], d],
            send_sem=a2_send.at[h],
            recv_sem=a2_recv.at[h, d // per],
            device_id={"expert": plus(e, -d)},
            device_id_type=MESH,
        )

    m = held * cap * n
    row_of = lax.broadcasted_iota(jnp.int32, (m, half), 0)
    lane_of = lax.broadcasted_iota(jnp.int32, (m, half), 1)
    meets = ((lane_of % SPAN) // 8 == row_of % n) & (lane_of // SPAN == row_of // (cap * n))
    wanted = jnp.where(meets, ((row_of // n) % cap + 1).astype(F32), -1.0)
    for h in range(2):
        bytes_of(toks.at[h, pl.ds(0, n - 1)], a1_recv.at[h])
        marks = jnp.zeros((8, half), F32)
        for b in range(n):
            marks = marks + toks[h, b].astype(F32)
        block = toks[h].reshape(8 * n, half)
        if 8 * n < SPAN:
            block = jnp.concatenate([block, jnp.zeros((SPAN - 8 * n, half), BF16)], axis=0)
        block = jnp.concatenate([block] * held, axis=0)
        pick = jnp.concatenate(
            [jnp.where(marks[6 + r : 7 + r, :] == wanted, 1.0, 0.0) for r in range(n // held)],
            axis=0,
        ).astype(BF16)
        found = jnp.dot(pick, block, preferred_element_type=F32)
        sel[h] = found.reshape(n, cap, n, half).astype(BF16)
        for d in range(1, n):
            a2(h, d).start()
        rows[h, :, wid[h], 0] = sel[h, e]

    def a3(h, s, way, k, j):
        step = 1 if way == 0 else -1
        base = 0 if k <= 2 else 2
        unit = rows.at[h, s, plus(wid[h], -step * base), pl.ds(j * per, per)]
        return pltpu.make_async_remote_copy(
            src_ref=unit,
            dst_ref=unit,
            send_sem=a3_send.at[h, s],
            recv_sem=a3_recv.at[h, s, way, k - 1, j],
            device_id={WIDE[h]: plus(wid[h], step * (k - base))},
            device_id_type=MESH,
        )

    def split(way, k, j, count):
        return k < top or (j < count // 2) == (way == 0)

    for j in range(CHUNKS):
        for h in range(2):
            count = per if j > 0 else per - 1
            if count > 0:
                bytes_of(sel.at[h, pl.ds(0, count)], a2_recv.at[h, j])
        for s in range(cap):
            for h in range(2):
                for way in range(2):
                    if top >= 2 and split(way, 2, j, CHUNKS):
                        a3(h, s, way, 2, j).start()
    for s in range(cap):
        for j in range(CHUNKS):
            for h in range(2):
                for way in range(2):
                    if split(way, 1, j, CHUNKS):
                        a3(h, s, way, 1, j).start()

    def pass_rows(s, k):
        for j in range(CHUNKS):
            for h in range(2):
                for way in range(2):
                    if split(way, k, j, CHUNKS):
                        a3(h, s, way, k, j).wait_recv()
                    for later in (4, 3) if k == 2 else ():
                        if later <= top and split(way, later, j, CHUNKS):
                            a3(h, s, way, later, j).start()

    order = [0]
    for d in range(1, top):
        order += [d, n - d]
    order.append(top)
    place = {d: p for p, d in enumerate(order)}

    def c1(h, s, d):
        send, to = (0, -d) if d != top else ((top - 1, -1) if s % 2 == 0 else ((1 - top) % n, 1))
        return pltpu.make_async_remote_copy(
            src_ref=hid.at[h, s, wid[h], place[send]],
            dst_ref=hid.at[h, s, wid[h], place[d]],
            send_sem=c1_send.at[h, s],
            recv_sem=c1_recv.at[h, s, d],
            device_id={NARROW[h]: plus(nar[h], to)},
            device_id_type=MESH,
        )

    def c2(h, s, way, k, i):
        step = 1 if way == 0 else -1
        unit = hid.at[h, s, plus(wid[h], -step * (k - 1)), pl.ds(2 * i, 2)]
        return pltpu.make_async_remote_copy(
            src_ref=unit,
            dst_ref=unit,
            send_sem=c2_send.at[h, s],
            recv_sem=c2_recv.at[h, s, way, k - 1, i],
            device_id={WIDE[h]: plus(wid[h], step)},
            device_id_type=MESH,
        )

    def project(s):
        sums = []
        for h in range(2):
            total = jnp.zeros((cells, 2 * hidden_units), F32)
            for d in range(n):
                at = pl.multiple_of(plus(e, d) * (2 * half) + h * half, half)
                lhs = rows[h, s, :, d].reshape(cells, half)
                rhs = jnp.concatenate(
                    [gate_w[pl.ds(at, half), :], up_w[pl.ds(at, half), :]], axis=1
                )
                total = total + jnp.dot(lhs, rhs, preferred_element_type=F32)
            sums.append(total)
        for c in range(2):
            part[c] = sums[0][:, c * hidden_units : (c + 1) * hidden_units]
        gated, up = (
            jnp.concatenate([part[c, pl.ds(b, n, stride=n), :] for b in range(n)], axis=0)
            + sums[1][:, c * hidden_units : (c + 1) * hidden_units]
            for c in range(2)
        )
        hidden = ((gated / (1.0 + jnp.exp(-gated))) * up).astype(BF16)
        for h in range(2):
            hid[h, s, wid[h], 0] = hidden[h * hcells : (h + 1) * hcells, :]

    def begin(s):
        project(s)
        for k in range(top - 1, 0, -1):
            for d in (k, n - k):
                for h in range(2):
                    c1(h, s, d).start()
        if top == 1:
            for h in range(2):
                c1(h, s, top).start()

    if top >= 2:
        for s in range(cap):
            pass_rows(s, 2)
    for copy in loads:
        copy.wait()
    for s in range(cap):
        for k in (1, 3, 4):
            if k <= top:
                pass_rows(s, k)
        begin(s)

    acc[...] = jnp.zeros_like(acc)
    pairs = n // 2

    def use(h, src, i):
        lhs, rhs = [], []
        for p in (2 * i, 2 * i + 1):
            other = plus(nar[h], order[p])
            unit = src * n + other if h == 0 else other * n + src
            at = pl.multiple_of(unit * hidden_units, hidden_units)
            lhs.append(hid[h, :, src, p].reshape(cap * hcells, hidden_units))
            rhs.append(down_w[:, :, pl.ds(at, hidden_units)].reshape(128, hidden_units))
        acc[h] += lax.dot_general(
            jnp.concatenate(lhs, axis=1),
            jnp.concatenate(rhs, axis=1),
            (((1,), (1,)), ((), ())),
            preferred_element_type=F32,
        )

    early = pairs - 1

    def use_step(t):
        for h in range(2):
            for i in range(pairs):
                k = t if i < early else t - 1
                if k == 0:
                    use(h, wid[h], i)
                elif 1 <= k < top:
                    use(h, plus(wid[h], -k), i)
                    use(h, plus(wid[h], k), i)
                elif k == top:
                    use(h, plus(wid[h], k), i)

    def launch(h, s, i):
        for way in range(2):
            if split(way, 1, i, pairs):
                c2(h, s, way, 1, i).start()

    def pass_hidden(h, s, k, i):
        for way in range(2):
            if split(way, k, i, pairs):
                c2(h, s, way, k, i).wait_recv()
            if k < top and split(way, k + 1, i, pairs):
                c2(h, s, way, k + 1, i).start()

    for s in range(cap):
        for h in range(2):
            for p in range(1, n - 1):
                c1(h, s, order[p]).wait_recv()
                if p % 2 == 1:
                    launch(h, s, p // 2)
                if top > 1 and order[p] == (top - 1 if s % 2 == 0 else n - top + 1):
                    c1(h, s, top).start()
    for t in range(1, top + 2):
        if t == top + 1:
            use_step(top)
        for s in range(cap):
            for h in range(2):
                for i in range(early if t <= top else 0):
                    pass_hidden(h, s, t, i)
                if t == 1:
                    c1(h, s, top).wait_recv()
                    launch(h, s, pairs - 1)
                else:
                    pass_hidden(h, s, t - 1, pairs - 1)
        if t <= top:
            use_step(t - 1)
    use_step(top + 1)

    def e1(d):
        return pltpu.make_async_remote_copy(
            src_ref=give.at[plus(z, -d)],
            dst_ref=got.at[z],
            send_sem=e1_send,
            recv_sem=e1_recv,
            device_id={"shard_1": plus(z, -d)},
            device_id_type=MESH,
        )

    for a in range(n):
        for s in range(cap):
            at = s * hcells + (a % top) * n
            give[a, s] = acc[a // top, at : at + n, :].astype(BF16)
    for d in far:
        e1(d).start()
    got[z] = give[z]

    at_tok = lax.broadcasted_iota(jnp.int32, (8, 128), 0)
    at_row = lax.broadcasted_iota(jnp.int32, (8, 128), 1)
    whose = jnp.where(at_row < n * cap, at_row // cap, -1)
    coefs = jnp.zeros((8, 128), F32)
    for t, code in enumerate(codes_of(whose)):
        weight = jnp.where(ids[0][t] == whose, amount[0][t], 0.0) + jnp.where(
            ids[1][t] == whose, amount[1][t], 0.0
        )
        mine = (at_tok == t) & (code == (at_row % cap + 1).astype(F32))
        coefs = jnp.where(mine, weight, coefs)

    for h in range(2):
        bytes_of(toks.at[h, pl.ds(0, n - 1)], a1_send.at[h])
        bytes_of(sel.at[h, pl.ds(0, n - 1)], a2_send.at[h])
        for s in range(cap):
            bytes_of(rows.at[h, s, pl.ds(0, n - 1)], a3_send.at[h, s])
            bytes_of(hid.at[h, s, 0, pl.ds(0, n - 1)], c1_send.at[h, s])
            bytes_of(hid.at[h, s, pl.ds(0, n - 1)], c2_send.at[h, s])
    bytes_of(give.at[pl.ds(0, n - 1)], e1_recv)
    got32[...] = got[...].astype(F32).reshape(got32.shape)
    for b in range(n):
        mine = got32[pl.ds(b, n * cap, stride=n), :]
        pass_on[b] = mine.reshape(cap, n, 128).astype(BF16)

    def e2(b, src):
        return pltpu.make_async_remote_copy(
            src_ref=pass_on.at[b],
            dst_ref=back.at[src],
            send_sem=e2_send,
            recv_sem=e2_recv,
            device_id={"expert": y, "shard_0": b},
            device_id_type=MESH,
        )

    for b in range(n):
        here = (e == y) & (y == b)

        @pl.when(jnp.logical_not(here))
        def _(b=b):
            e2(b, e).start()

        @pl.when(here)
        def _(b=b):
            back[e] = pass_on[b]

    @pl.when(e == y)
    def _():
        bytes_of(back.at[pl.ds(0, n - 1)], e2_recv)

    @pl.when(e != y)
    def _():
        bytes_of(back, e2_recv)

    low = lax.broadcasted_iota(jnp.int32, (1, 128), 1) < 64
    sums = [jnp.zeros((8, 128), F32) for _ in range(n // 2)]
    for src in range(n):
        value = back[src].astype(F32).reshape(n * cap, 128)
        for s in range(cap):
            at = src * cap + s
            coef = coefs[:, at : at + 1]
            for g in range(n // 2):
                a, b = 2 * g * cap + s, (2 * g + 1) * cap + s
                sums[g] = sums[g] + coef * jnp.where(low, value[a : a + 1, :], value[b : b + 1, :])
    for g in range(n // 2):
        out_ref[:, g * 128 : (g + 1) * 128] = sums[g][:tok_count, :].astype(BF16)

    bytes_of(give.at[pl.ds(0, n - 1)], e1_send)

    @pl.when(e == y)
    def _():
        bytes_of(pass_on.at[pl.ds(0, n - 1)], e2_send)

    @pl.when(e != y)
    def _():
        bytes_of(pass_on, e2_send)


def shards(n, tokens, expert_ids, gates, gate_proj, up_proj, down_proj_t):
    tok_count, feats = tokens.shape
    half = feats // 2
    hidden_units = gate_proj.shape[2]
    out_feats = down_proj_t.shape[1]
    cap = min(tok_count, 4 * tok_count // n)
    cells = n * n
    top = n // 2
    dma = pltpu.SemaphoreType.DMA
    vmem = pltpu.VMEM
    return pl.pallas_call(
        functools.partial(kernel, n, cap),
        out_shape=jax.ShapeDtypeStruct((tok_count, feats), BF16),
        in_specs=[pl.BlockSpec(memory_space=pl.ANY)] * 6,
        out_specs=pl.BlockSpec(memory_space=vmem),
        scratch_shapes=[
            vmem(tokens.shape, BF16),
            vmem((2, tok_count), jnp.int32),
            vmem((2, tok_count), F32),
            vmem((8, feats), F32),
            vmem((2, n, 8, half), BF16),
            vmem((2, n, cap, n, half), BF16),
            vmem((2, cap, n, n, n, half), BF16),
            vmem((2, cells, hidden_units), F32),
            vmem((2, cap, n, n, cells // 2, hidden_units), BF16),
            vmem((2, cap * cells // 2, 128), F32),
            vmem((n, cap, n, 128), BF16),
            vmem((n, cap, n, 128), BF16),
            vmem((n * cap * n, 128), F32),
            vmem((n, cap, n, 128), BF16),
            vmem((n, cap, n, 128), BF16),
            vmem(gate_proj.shape[1:], BF16),
            vmem(up_proj.shape[1:], BF16),
            vmem((2, out_feats, down_proj_t.shape[2]), BF16),
            dma((7,)),
            dma((2,)), dma((2,)),
            dma((2,)), dma((2, CHUNKS)),
            dma((2, cap)), dma((2, cap, 2, top, CHUNKS)),
            dma((2, cap)), dma((2, cap, n)),
            dma((2, cap)), dma((2, cap, 2, top, n // 2)),
            dma, dma,
            dma, dma,
        ],
        compiler_params=pltpu.CompilerParams(collective_id=0, has_side_effects=True),
        name="experts",
    )(tokens, expert_ids.T, gates.T, gate_proj[0], up_proj[0], down_proj_t[0])


def solution(mesh):
    n = mesh.shape["expert"]
    split = Mesh(mesh.devices.reshape(n, n, n), ("expert", "shard_0", "shard_1"))
    placed = (
        P(SHARD, "expert"),
        P(SHARD, None),
        P(SHARD, None),
        P("expert", None, SHARD),
        P("expert", None, SHARD),
        P("expert", SHARD, None),
    )
    return jax.shard_map(
        functools.partial(shards, n),
        mesh=split,
        in_specs=placed,
        out_specs=P(SHARD, "expert"),
        check_vma=False,
    )
```

```python
import functools

import jax
import jax.numpy as jnp
from jax import lax
from jax.experimental import pallas as pl
from jax.experimental.pallas import tpu as pltpu
from jax.sharding import Mesh
from jax.sharding import PartitionSpec as P

SHARD = ("shard_0", "shard_1")
MESH = pl.DeviceIdType.MESH
NARROW = ("shard_1", "shard_0")
WIDE = ("shard_0", "shard_1")
CHUNKS = 2
SPAN = 64
F32, BF16 = jnp.float32, jnp.bfloat16


def kernel(
    n, cap, tok_hbm, ids_hbm, gates_hbm, gate_hbm, up_hbm, down_hbm, out_ref,
    tok_v, ids_v, gates_v, stage, toks, sel, rows, part, hid, acc, give, got, got32, pass_on, back,
    gate_w, up_w, down_w,
    load_sem, a1_send, a1_recv, a2_send, a2_recv, a3_send, a3_recv, a3_rest,
    c1_send, c1_recv, c2_send, c2_recv, e1_send, e1_recv, e2_send, e2_recv,
):
    e = lax.axis_index("expert")
    y = lax.axis_index("shard_0")
    z = lax.axis_index("shard_1")
    nar = (z, y)
    wid = (y, z)
    top = n // 2
    cells = n * n
    hcells = cells // 2
    tok_count, feats = tok_v.shape
    half = feats // 2
    hidden_units = gate_w.shape[1]
    per = n // CHUNKS
    far = [d for k in range(top) for d in sorted({top - k, top + k}) if d < n]

    def plus(a, b):
        return lax.rem(a + b + n, n)

    small = [
        pltpu.make_async_copy(ids_hbm, ids_v, load_sem.at[0]),
        pltpu.make_async_copy(gates_hbm, gates_v, load_sem.at[1]),
        pltpu.make_async_copy(tok_hbm, tok_v, load_sem.at[2]),
    ]
    loads = [
        pltpu.make_async_copy(gate_hbm, gate_w, load_sem.at[3]),
        pltpu.make_async_copy(up_hbm, up_w, load_sem.at[4]),
        pltpu.make_async_copy(down_hbm, down_w.at[0], load_sem.at[5]),
        pltpu.make_async_copy(down_hbm, down_w.at[1], load_sem.at[6]),
    ]
    for copy in small:
        copy.start()
    barrier = pltpu.get_barrier_semaphore()
    for d in far:
        for axis, own in (("shard_1", z), ("shard_0", y), ("expert", e)):
            pl.semaphore_signal(
                barrier, inc=1, device_id={axis: plus(own, d)}, device_id_type=MESH
            )
    for copy in small:
        copy.wait()
    for copy in loads:
        copy.start()

    ids = [[ids_v[k : k + 1, t : t + 1] for t in range(tok_count)] for k in range(2)]
    amount = [[gates_v[k : k + 1, t : t + 1] for t in range(tok_count)] for k in range(2)]

    def codes_of(expert):
        run = jnp.zeros(expert.shape, F32)
        out = []
        for t in range(tok_count):
            hit = (ids[0][t] == expert) | (ids[1][t] == expert)
            out.append(jnp.where(hit, run + 1.0, 0.0))
            run = run + jnp.where(hit, 1.0, 0.0)
        return out

    sub = lax.broadcasted_iota(jnp.int32, (8, half), 0)
    lane = lax.broadcasted_iota(jnp.int32, (8, half), 1)
    held = half // SPAN
    expert = jnp.where(sub >= 6, (sub - 6) * held + lane // SPAN, -1)
    codes = codes_of(expert)
    stage[...] = jnp.zeros_like(stage)
    stage[0:tok_count, :] = tok_v[...].astype(F32)
    for h in range(2):
        here = (lane % SPAN) // 8 == nar[h]
        spare = jnp.zeros((8, half), F32)
        for t in range(tok_count):
            spare = jnp.where(here & (lane % 8 == t), codes[t], spare)
        toks[h, nar[h]] = (stage[:, h * half : (h + 1) * half] + spare).astype(BF16)

    pl.semaphore_wait(barrier, 3 * (n - 1))

    def bytes_of(ref, sem):
        return pltpu.make_async_copy(ref, ref, sem).wait()

    def a1(h, d):
        block = toks.at[h, nar[h]]
        return pltpu.make_async_remote_copy(
            src_ref=block,
            dst_ref=block,
            send_sem=a1_send.at[h],
            recv_sem=a1_recv.at[h],
            device_id={NARROW[h]: plus(nar[h], -d)},
            device_id_type=MESH,
        )

    for d in far:
        for h in range(2):
            a1(h, d).start()

    def a2(h, d):
        return pltpu.make_async_remote_copy(
            src_ref=sel.at[h, plus(e, -d)],
            dst_ref=rows.at[h, :, wid[h], d],
            send_sem=a2_send.at[h],
            recv_sem=a2_recv.at[h, d // per],
            device_id={"expert": plus(e, -d)},
            device_id_type=MESH,
        )

    m = held * cap * n
    row_of = lax.broadcasted_iota(jnp.int32, (m, half), 0)
    lane_of = lax.broadcasted_iota(jnp.int32, (m, half), 1)
    meets = ((lane_of % SPAN) // 8 == row_of % n) & (lane_of // SPAN == row_of // (cap * n))
    wanted = jnp.where(meets, ((row_of // n) % cap + 1).astype(F32), -1.0)
    for h in range(2):
        bytes_of(toks.at[h, pl.ds(0, n - 1)], a1_recv.at[h])
        marks = jnp.zeros((8, half), F32)
        for b in range(n):
            marks = marks + toks[h, b].astype(F32)
        block = toks[h].reshape(8 * n, half)
        if 8 * n < SPAN:
            block = jnp.concatenate([block, jnp.zeros((SPAN - 8 * n, half), BF16)], axis=0)
        block = jnp.concatenate([block] * held, axis=0)
        pick = jnp.concatenate(
            [jnp.where(marks[6 + r : 7 + r, :] == wanted, 1.0, 0.0) for r in range(n // held)],
            axis=0,
        ).astype(BF16)
        found = jnp.dot(pick, block, preferred_element_type=F32)
        sel[h] = found.reshape(n, cap, n, half).astype(BF16)
        for d in range(1, n):
            a2(h, d).start()
        rows[h, :, wid[h], 0] = sel[h, e]

    def a3(h, s, way, k, j):
        step = 1 if way == 0 else -1
        base = 0 if k <= 2 else 2
        unit = rows.at[h, s, plus(wid[h], -step * base), pl.ds(j * per, per)]
        return pltpu.make_async_remote_copy(
            src_ref=unit,
            dst_ref=unit,
            send_sem=a3_send.at[h, s],
            recv_sem=a3_recv.at[h, s, way, j] if k == 2 else a3_rest.at[h, s],
            device_id={WIDE[h]: plus(wid[h], step * (k - base))},
            device_id_type=MESH,
        )

    def split(way, k, j, count):
        return k < top or (j < count // 2) == (way == 0)

    for j in range(CHUNKS):
        for h in range(2):
            count = per if j > 0 else per - 1
            if count > 0:
                bytes_of(sel.at[h, pl.ds(0, count)], a2_recv.at[h, j])
        for s in range(cap):
            for h in range(2):
                for way in range(2):
                    if top >= 2 and split(way, 2, j, CHUNKS):
                        a3(h, s, way, 2, j).start()
    for s in range(cap):
        for j in range(CHUNKS):
            for h in range(2):
                for way in range(2):
                    if split(way, 1, j, CHUNKS):
                        a3(h, s, way, 1, j).start()

    def pass_rows(s):
        for j in range(CHUNKS):
            for h in range(2):
                for way in range(2):
                    if split(way, 2, j, CHUNKS):
                        a3(h, s, way, 2, j).wait_recv()
                    for later in (4, 3):
                        if later <= top and split(way, later, j, CHUNKS):
                            a3(h, s, way, later, j).start()

    order = [0]
    for d in range(1, top):
        order += [d, n - d]
    order.append(top)
    place = {d: p for p, d in enumerate(order)}

    def c1(h, s, d):
        send, to = (0, -d) if d != top else ((top - 1, -1) if s % 2 == 0 else ((1 - top) % n, 1))
        return pltpu.make_async_remote_copy(
            src_ref=hid.at[h, s, wid[h], place[send]],
            dst_ref=hid.at[h, s, wid[h], place[d]],
            send_sem=c1_send.at[h, s],
            recv_sem=c1_recv.at[h, s, pairs if d == top else place[d] // 2],
            device_id={NARROW[h]: plus(nar[h], to)},
            device_id_type=MESH,
        )

    def c2(h, s, way, k, i):
        step = 1 if way == 0 else -1
        unit = hid.at[h, s, plus(wid[h], -step * (k - 1)), pl.ds(2 * i, 2)]
        return pltpu.make_async_remote_copy(
            src_ref=unit,
            dst_ref=unit,
            send_sem=c2_send.at[h, s],
            recv_sem=c2_recv.at[h, s, way, k - 1, i],
            device_id={WIDE[h]: plus(wid[h], step)},
            device_id_type=MESH,
        )

    def project(s):
        sums = []
        for h in range(2):
            total = jnp.zeros((cells, 2 * hidden_units), F32)
            for d in range(n):
                at = pl.multiple_of(plus(e, d) * (2 * half) + h * half, half)
                lhs = rows[h, s, :, d].reshape(cells, half)
                rhs = jnp.concatenate(
                    [gate_w[pl.ds(at, half), :], up_w[pl.ds(at, half), :]], axis=1
                )
                total = total + jnp.dot(lhs, rhs, preferred_element_type=F32)
            sums.append(total)
        for c in range(2):
            part[c] = sums[0][:, c * hidden_units : (c + 1) * hidden_units]
        gated, up = (
            jnp.concatenate([part[c, pl.ds(b, n, stride=n), :] for b in range(n)], axis=0)
            + sums[1][:, c * hidden_units : (c + 1) * hidden_units]
            for c in range(2)
        )
        hidden = ((gated / (1.0 + jnp.exp(-gated))) * up).astype(BF16)
        for h in range(2):
            hid[h, s, wid[h], 0] = hidden[h * hcells : (h + 1) * hcells, :]

    def begin(s):
        project(s)
        for k in range(top - 1, 0, -1):
            for d in (k, n - k):
                for h in range(2):
                    c1(h, s, d).start()
        if top == 1:
            for h in range(2):
                c1(h, s, top).start()

    if top >= 2:
        for s in range(cap):
            pass_rows(s)
    for copy in loads:
        copy.wait()
    for s in range(cap):
        for h in range(2):
            units = n - 1 - (2 if top > 2 else 1 if top == 2 else 0)
            bytes_of(rows.at[h, s, pl.ds(0, units)], a3_rest.at[h, s])
        begin(s)

    acc[...] = jnp.zeros_like(acc)
    pairs = n // 2

    def use(h, src, i):
        lhs, rhs = [], []
        for p in (2 * i, 2 * i + 1):
            other = plus(nar[h], order[p])
            unit = src * n + other if h == 0 else other * n + src
            at = pl.multiple_of(unit * hidden_units, hidden_units)
            lhs.append(hid[h, :, src, p].reshape(cap * hcells, hidden_units))
            rhs.append(down_w[:, :, pl.ds(at, hidden_units)].reshape(128, hidden_units))
        acc[h] += lax.dot_general(
            jnp.concatenate(lhs, axis=1),
            jnp.concatenate(rhs, axis=1),
            (((1,), (1,)), ((), ())),
            preferred_element_type=F32,
        )

    early = pairs - 1

    def use_step(t):
        for h in range(2):
            for i in range(pairs):
                k = t if i < early else t - 1
                if k == 0:
                    use(h, wid[h], i)
                elif 1 <= k < top:
                    use(h, plus(wid[h], -k), i)
                    use(h, plus(wid[h], k), i)
                elif k == top:
                    use(h, plus(wid[h], k), i)

    def launch(h, s, i):
        for way in range(2):
            if split(way, 1, i, pairs):
                c2(h, s, way, 1, i).start()

    def pass_hidden(h, s, k, i):
        for way in range(2):
            if split(way, k, i, pairs):
                c2(h, s, way, k, i).wait_recv()
            if k < top and split(way, k + 1, i, pairs):
                c2(h, s, way, k + 1, i).start()

    for s in range(cap):
        for i in range(pairs):
            for h in range(2):
                count = sum(1 for p in (2 * i, 2 * i + 1) if order[p] not in (0, top))
                if count:
                    bytes_of(hid.at[h, s, 0, pl.ds(0, count)], c1_recv.at[h, s, i])
                if i < early:
                    launch(h, s, i)
                if top > 1 and place[top - 1 if s % 2 == 0 else n - top + 1] // 2 == i:
                    c1(h, s, top).start()
    for t in range(1, top + 2):
        if t == top + 1:
            use_step(top)
        for s in range(cap):
            for h in range(2):
                for i in range(early if t <= top else 0):
                    pass_hidden(h, s, t, i)
                if t == 1:
                    c1(h, s, top).wait_recv()
                    launch(h, s, pairs - 1)
                else:
                    pass_hidden(h, s, t - 1, pairs - 1)
        if t <= top:
            use_step(t - 1)
    use_step(top + 1)

    def e1(d):
        return pltpu.make_async_remote_copy(
            src_ref=give.at[plus(z, -d)],
            dst_ref=got.at[z],
            send_sem=e1_send,
            recv_sem=e1_recv,
            device_id={"shard_1": plus(z, -d)},
            device_id_type=MESH,
        )

    for a in range(n):
        for s in range(cap):
            at = s * hcells + (a % top) * n
            give[a, s] = acc[a // top, at : at + n, :].astype(BF16)
    for d in far:
        e1(d).start()
    got[z] = give[z]

    at_tok = lax.broadcasted_iota(jnp.int32, (8, 128), 0)
    at_row = lax.broadcasted_iota(jnp.int32, (8, 128), 1)
    whose = jnp.where(at_row < n * cap, at_row // cap, -1)
    coefs = jnp.zeros((8, 128), F32)
    for t, code in enumerate(codes_of(whose)):
        weight = jnp.where(ids[0][t] == whose, amount[0][t], 0.0) + jnp.where(
            ids[1][t] == whose, amount[1][t], 0.0
        )
        mine = (at_tok == t) & (code == (at_row % cap + 1).astype(F32))
        coefs = jnp.where(mine, weight, coefs)

    for h in range(2):
        bytes_of(toks.at[h, pl.ds(0, n - 1)], a1_send.at[h])
        bytes_of(sel.at[h, pl.ds(0, n - 1)], a2_send.at[h])
        for s in range(cap):
            bytes_of(rows.at[h, s, pl.ds(0, n - 1)], a3_send.at[h, s])
            bytes_of(hid.at[h, s, 0, pl.ds(0, n - 1)], c1_send.at[h, s])
            bytes_of(hid.at[h, s, pl.ds(0, n - 1)], c2_send.at[h, s])
    bytes_of(give.at[pl.ds(0, n - 1)], e1_recv)
    got32[...] = got[...].astype(F32).reshape(got32.shape)
    for b in range(n):
        mine = got32[pl.ds(b, n * cap, stride=n), :]
        pass_on[b] = mine.reshape(cap, n, 128).astype(BF16)

    def e2(b, src):
        return pltpu.make_async_remote_copy(
            src_ref=pass_on.at[b],
            dst_ref=back.at[src],
            send_sem=e2_send,
            recv_sem=e2_recv,
            device_id={"expert": y, "shard_0": b},
            device_id_type=MESH,
        )

    for b in range(n):
        here = (e == y) & (y == b)

        @pl.when(jnp.logical_not(here))
        def _(b=b):
            e2(b, e).start()

        @pl.when(here)
        def _(b=b):
            back[e] = pass_on[b]

    @pl.when(e == y)
    def _():
        bytes_of(back.at[pl.ds(0, n - 1)], e2_recv)

    @pl.when(e != y)
    def _():
        bytes_of(back, e2_recv)

    low = lax.broadcasted_iota(jnp.int32, (1, 128), 1) < 64
    sums = [jnp.zeros((8, 128), F32) for _ in range(n // 2)]
    for src in range(n):
        value = back[src].astype(F32).reshape(n * cap, 128)
        for s in range(cap):
            at = src * cap + s
            coef = coefs[:, at : at + 1]
            for g in range(n // 2):
                a, b = 2 * g * cap + s, (2 * g + 1) * cap + s
                sums[g] = sums[g] + coef * jnp.where(low, value[a : a + 1, :], value[b : b + 1, :])
    for g in range(n // 2):
        out_ref[:, g * 128 : (g + 1) * 128] = sums[g][:tok_count, :].astype(BF16)

    bytes_of(give.at[pl.ds(0, n - 1)], e1_send)

    @pl.when(e == y)
    def _():
        bytes_of(pass_on.at[pl.ds(0, n - 1)], e2_send)

    @pl.when(e != y)
    def _():
        bytes_of(pass_on, e2_send)


def shards(n, tokens, expert_ids, gates, gate_proj, up_proj, down_proj_t):
    tok_count, feats = tokens.shape
    half = feats // 2
    hidden_units = gate_proj.shape[2]
    out_feats = down_proj_t.shape[1]
    cap = min(tok_count, 4 * tok_count // n)
    cells = n * n
    top = n // 2
    dma = pltpu.SemaphoreType.DMA
    vmem = pltpu.VMEM
    return pl.pallas_call(
        functools.partial(kernel, n, cap),
        out_shape=jax.ShapeDtypeStruct((tok_count, feats), BF16),
        in_specs=[pl.BlockSpec(memory_space=pl.ANY)] * 6,
        out_specs=pl.BlockSpec(memory_space=vmem),
        scratch_shapes=[
            vmem(tokens.shape, BF16),
            vmem((2, tok_count), jnp.int32),
            vmem((2, tok_count), F32),
            vmem((8, feats), F32),
            vmem((2, n, 8, half), BF16),
            vmem((2, n, cap, n, half), BF16),
            vmem((2, cap, n, n, n, half), BF16),
            vmem((2, cells, hidden_units), F32),
            vmem((2, cap, n, n, cells // 2, hidden_units), BF16),
            vmem((2, cap * cells // 2, 128), F32),
            vmem((n, cap, n, 128), BF16),
            vmem((n, cap, n, 128), BF16),
            vmem((n * cap * n, 128), F32),
            vmem((n, cap, n, 128), BF16),
            vmem((n, cap, n, 128), BF16),
            vmem(gate_proj.shape[1:], BF16),
            vmem(up_proj.shape[1:], BF16),
            vmem((2, out_feats, down_proj_t.shape[2]), BF16),
            dma((7,)),
            dma((2,)), dma((2,)),
            dma((2,)), dma((2, CHUNKS)),
            dma((2, cap)), dma((2, cap, 2, CHUNKS)), dma((2, cap)),
            dma((2, cap)), dma((2, cap, n // 2 + 1)),
            dma((2, cap)), dma((2, cap, 2, top, n // 2)),
            dma, dma,
            dma, dma,
        ],
        compiler_params=pltpu.CompilerParams(collective_id=0, has_side_effects=True),
        name="experts",
    )(tokens, expert_ids.T, gates.T, gate_proj[0], up_proj[0], down_proj_t[0])


def solution(mesh):
    n = mesh.shape["expert"]
    split = Mesh(mesh.devices.reshape(n, n, n), ("expert", "shard_0", "shard_1"))
    placed = (
        P(SHARD, "expert"),
        P(SHARD, None),
        P(SHARD, None),
        P("expert", None, SHARD),
        P("expert", None, SHARD),
        P("expert", SHARD, None),
    )
    return jax.shard_map(
        functools.partial(shards, n),
        mesh=split,
        in_specs=placed,
        out_specs=P(SHARD, "expert"),
        check_vma=False,
    )
```
